256 devices in a mesh: groups: 2 (over z), band: 64 (over y, x), sub: 2 (over core).
Axes of the slice: x: 8, y: 8, z: 2, core: 2. Of those that a mesh axis runs over, the one named last changes fastest.
The devices are a block of a 8x8x16 slice.
Arguments:
- sky_maps: bfloat16 [256, 2, 32, 16384], P(('groups', 'band', 'sub')), parts along dimension 0, may hold values from -6 to 6
- sky_mask: float32 [256, 16384], P(('groups', 'band', 'sub')), parts along dimension 0, may hold values from 0.005 to 1, as said below
- pixel_counts: int32 [256], P(('groups', 'band', 'sub')), parts along dimension 0, may hold values from 8192 to 16384, as said below
- phi_offsets: int32 [256], P(('groups', 'band', 'sub')), parts along dimension 0, may hold values from 0 to 1
- low_orders: int32 [256], P('groups'), parts along dimension 0, may hold values from 1 to 4095, as said below
- legendre: bfloat16 [256, 8192, 256], P(('groups', 'band', 'sub')), parts along dimension 0, may hold values from -0.375 to 0.375
Outputs:
- alm_packed: float32 [256, 8192, 128], P(('groups', 'band', 'sub')), parts along dimension 0
- spectra: float32 [16384, 2, 1024], P(('groups', 'band', 'sub')), parts along dimension 0
The draws below stay inside these ranges and needn't reach their ends.
There are 2 independent parts, one for each index of `groups`. The reference program is written for one: setup_inputs(seed, part) draws one part's arguments, and reference() takes and returns one part's arrays. A program takes and returns all parts, laid end to end along the dimension named above; each array names one. Nothing has to cross between parts.
Inputs may be any that keep to these rules, and one draw needn't show every extreme that they name: `pixel_counts`: multiples of 4; some cycle has exactly 16384 pixels; pixel slots at or past a cycle's count are not used. `low_orders`: all distinct. `sky_mask`: Positive.
All inputs are finite; a program needn't handle non-finite values.
Results may differ from the reference program's by a relative error of at most 0.0046.
Values may be sent and summed in bfloat16 or wider, within the bound.
No kernel may reach another device: no remote copies, remote signals or barrier semaphores. Data moves between devices by JAX's collectives and lax.ppermute only.
A program may use at most 64 MiB of HBM per device.

```python
import math
import jax
import jax.numpy as jnp
from jax import lax

LMAX = 8192
PIXMAX = 16384
MAPS = 32
CYCLES = 128
PAIRS = 128


def draw_pixel_counts(key, part):
    quarters = jax.random.randint(key, (CYCLES,), PIXMAX // 8, PIXMAX // 4 + 1)
    counts = 4 * quarters
    longest = jax.random.randint(jax.random.fold_in(key, 7), (), 0, CYCLES)
    counts = jnp.where(jnp.arange(CYCLES) == longest, PIXMAX, counts)
    return counts.astype(jnp.int32)


def draw_low_orders(key, part):
    shuffled = jax.random.permutation(key, LMAX // 2 - 1)
    return (shuffled[:PAIRS] + 1).astype(jnp.int32)


def draw_sky_mask(key, part):
    position = jnp.arange(CYCLES, dtype=jnp.float32) / max(CYCLES - 1, 1)
    cycle_level = 10.0 ** (-0.5 + 0.5 * position)
    pixel_noise = jax.random.uniform(key, (CYCLES, PIXMAX), jnp.float32, 0.3, 1.0)
    return (cycle_level[:, None] * pixel_noise).astype(jnp.float32)


def set_ends(result, rng, smallest, largest):
    dims = result.shape
    place = [jax.random.randint(jax.random.fold_in(rng, axis), (), 0, dims[axis]) for axis in range(len(dims))]
    result = result.at[tuple(place)].set(smallest)
    longest = dims.index(max(dims))
    place[longest] = (place[longest] + 1) % dims[longest]
    return result.at[tuple(place)].set(largest)


def level_of(own_key, shape, pieces, low, top_value):
    gain = 1.0
    for dim, parts in pieces:
        draws = jax.random.uniform(jax.random.fold_in(jax.random.fold_in(own_key, 6), dim), (parts,), jnp.float32, low / len(pieces), top_value / len(pieces))
        gain = gain * jnp.repeat(jnp.exp(draws), shape[dim] // parts).reshape((-1,) + (1,) * (len(shape) - 1 - dim))
    return gain


def gaussian(key, shape, spread, most, pieces=(), kind=jnp.bfloat16):
    values = jax.random.normal(key, shape, jnp.float32) * spread
    if len(pieces) > 0:
        values = level_of(key, shape, pieces, -0.22, 0.18) * values
    return jnp.clip(values, min=-most, max=most).astype(kind)


def setup_inputs(seed: int = 0, part: int = 0) -> dict:
    key_of = jax.random.split(jax.random.key(seed), 7)
    part_keys = jax.random.split(jax.random.fold_in(key_of[6], part), 7)
    sky_maps = gaussian(part_keys[0], (CYCLES, 2, MAPS, PIXMAX), 1.0, 6.0, ((0, 128),))
    sky_mask = draw_sky_mask(jax.random.fold_in(jax.random.fold_in(key_of[6], part), 71), part)
    pixel_counts = draw_pixel_counts(jax.random.fold_in(jax.random.fold_in(key_of[6], part), 71), part)
    phi_offsets = set_ends(jax.random.randint(part_keys[3], (CYCLES,), 0, 2), jax.random.fold_in(part_keys[3], 1), 0, 1).astype(jnp.int32)
    low_orders = draw_low_orders(jax.random.fold_in(jax.random.fold_in(key_of[6], part), 71), part)
    legendre = gaussian(part_keys[5], (PAIRS, LMAX, 2 * CYCLES), (2 * CYCLES) ** -0.5, 0.375, ((0, 128),))
    return dict(sky_maps=sky_maps, sky_mask=sky_mask, pixel_counts=pixel_counts, phi_offsets=phi_offsets, low_orders=low_orders, legendre=legendre)


def slot_orders(low_orders):
    return jnp.stack([low_orders, LMAX - low_orders], axis=1).reshape(-1)

def finish_cycle(pixel_sums, cycle_count, orders):
    slots = orders.shape[0]
    maps_count = pixel_sums.shape[1] // 2
    inverse_root = 1.0 / jnp.sqrt(cycle_count.astype(jnp.float32))
    real_part = (pixel_sums[:slots] * inverse_root).reshape(slots, 2, maps_count)
    imag_part = (-pixel_sums[slots:] * inverse_root).reshape(slots, 2, maps_count)
    joined = jnp.stack([real_part[:, 0], imag_part[:, 0], real_part[:, 1], imag_part[:, 1]], axis=1).reshape(slots, 4 * maps_count)
    live_slots = 2 * orders < cycle_count
    return jnp.where(live_slots[:, None], joined, 0.0).astype(jnp.bfloat16)

def cycle_fourier(cycle_maps, cycle_mask, cycle_count, cycle_offset, orders):
    pixels = jnp.arange(PIXMAX, dtype=jnp.int32)
    cycle_rows = cycle_maps.reshape(2 * MAPS, PIXMAX).astype(jnp.float32)
    masked = jnp.where(pixels[None, :] < cycle_count, cycle_mask[None, :] * cycle_rows, 0.0).astype(jnp.bfloat16)
    phase_units = (2 * orders[:, None] * pixels[None, :] + orders[:, None] * cycle_offset) % (2 * cycle_count)
    phase_angle = jnp.pi * phase_units.astype(jnp.float32) / cycle_count.astype(jnp.float32)
    tables = jnp.concatenate([jnp.cos(phase_angle).astype(jnp.bfloat16), jnp.sin(phase_angle).astype(jnp.bfloat16)], axis=0)
    pixel_sums = jnp.dot(tables, masked.T, preferred_element_type=jnp.float32)
    return finish_cycle(pixel_sums, cycle_count, orders)

def stacked_operand(block_rows):
    quarter = block_rows.shape[1] // 4
    q_real = block_rows[:, :quarter]
    q_imag = block_rows[:, quarter:2 * quarter]
    u_real = block_rows[:, 2 * quarter:3 * quarter]
    u_imag = block_rows[:, 3 * quarter:]
    lower_half = jnp.concatenate([u_imag, -u_real, -q_imag, q_real], axis=1)
    return jnp.concatenate([block_rows, lower_half], axis=0)

def pair_alm(legendre_rows, first_order, first_block, second_block):
    both_operands = jnp.concatenate([stacked_operand(first_block), stacked_operand(second_block)], axis=1)
    product = -jnp.dot(legendre_rows, both_operands, preferred_element_type=jnp.float32)
    columns = first_block.shape[1]
    degree_count = legendre_rows.shape[0]
    degrees = jnp.arange(degree_count, dtype=jnp.int32)
    alm_rows = jnp.where((degrees < degree_count - first_order)[:, None], product[:, :columns], product[:, columns:])
    first_dense = jnp.where((degrees >= first_order)[:, None], jnp.roll(alm_rows, first_order, axis=0), 0.0).astype(jnp.bfloat16)
    second_dense = jnp.where((degrees >= degree_count - first_order)[:, None], alm_rows, 0.0).astype(jnp.bfloat16)
    return (alm_rows, jnp.stack([first_dense, second_dense], axis=0))

def reference(sky_maps, sky_mask, pixel_counts, phi_offsets, low_orders, legendre):
    orders = slot_orders(low_orders)

    def one_cycle(items):
        return cycle_fourier(items[0], items[1], items[2], items[3], orders)
    coefficients = lax.map(one_cycle, (sky_maps, sky_mask, pixel_counts, phi_offsets))
    by_slot = jnp.transpose(coefficients, (1, 0, 2)).reshape(PAIRS, 2, CYCLES, 4 * MAPS)

    def one_pair(items):
        return pair_alm(items[0], items[1], items[2][0], items[2][1])
    alm_packed, dense_pairs = lax.map(one_pair, (legendre, low_orders, by_slot))
    dense_rows = dense_pairs.reshape(2 * PAIRS, LMAX, 4 * MAPS)
    valid_pixels = jnp.arange(PIXMAX, dtype=jnp.int32)[None, :] < pixel_counts[:, None]
    weight = jnp.sum(jnp.where(valid_pixels, sky_mask * sky_mask, 0.0)) / jnp.sum(pixel_counts.astype(jnp.float32))
    block_rows = math.gcd(LMAX, 512)

    def spectra_block(first_degree):
        part_rows = lax.dynamic_slice_in_dim(dense_rows, first_degree, block_rows, 1).astype(jnp.float32)
        part_rows = part_rows.reshape(2 * PAIRS, block_rows, 2, 2, MAPS)
        totals = jnp.einsum('slerm,slern->lemn', part_rows, part_rows)
        degrees = first_degree + jnp.arange(block_rows, dtype=jnp.int32)
        counts = jnp.maximum(lax.optimization_barrier(jnp.sum((orders[None, :] <= degrees[:, None]).astype(jnp.int32), axis=1)), 1).astype(jnp.float32)
        return (2.0 * totals / (weight * counts)[:, None, None, None]).reshape(block_rows, 2, MAPS * MAPS)
    firsts = jnp.arange(LMAX // block_rows, dtype=jnp.int32) * block_rows
    spectra = lax.map(spectra_block, firsts).reshape(LMAX, 2, MAPS * MAPS)
    return (alm_packed, spectra)
```

```python
import functools

import jax
import jax.numpy as jnp
from jax import lax
from jax.experimental import pallas as pl
from jax.experimental.pallas import tpu as pltpu
from jax.sharding import Mesh
from jax.sharding import PartitionSpec as P

BAND_SUB = ("band_0", "band_1", "sub")
GROUPS_BAND_SUB = ("groups", "band_0", "band_1", "sub")

FINE = 256
GROUP = 8
VMEM_SPEC = pl.BlockSpec(memory_space=pltpu.VMEM)
SMEM_SPEC = pl.BlockSpec(memory_space=pltpu.SMEM)


def mod_units(units, modulus, inverse):
    quotient = jnp.floor(units.astype(jnp.float32) * inverse).astype(jnp.int32)
    rest = units - quotient * modulus
    rest = jnp.where(rest < 0, rest + modulus, rest)
    return jnp.where(rest >= modulus, rest - modulus, rest)


def turn(units, modulus, inverse, scale):
    angle = scale * mod_units(units, modulus, inverse).astype(jnp.float32)
    return jnp.cos(angle), jnp.sin(angle)


def combine(first, second):
    (a_cos, a_sin), (b_cos, b_sin) = first, second
    return a_cos * b_cos - a_sin * b_sin, a_sin * b_cos + a_cos * b_sin


def fourier_kernel(
    count_ref, offset_ref, orders_ref, mask_ref, maps_ref, coef_ref, sums_ref, table_ref, outer_ref, rows_ref
):
    pixel_slots = maps_ref.shape[1]
    rows = maps_ref.shape[0]
    maps_count = rows // 2
    slots = orders_ref.shape[1]
    count = count_ref[0]
    offset = offset_ref[0]
    count_float = count.astype(jnp.float32)
    modulus = 2 * count
    inverse = 1.0 / modulus.astype(jnp.float32)
    scale = jnp.pi / count_float
    orders = orders_ref[...]
    twice = 2 * orders
    coarse = pixel_slots // FINE
    near = 16
    step = lax.broadcasted_iota(jnp.int32, (near, slots), 0)
    low = turn(twice * step, modulus, inverse, scale)
    high = turn(twice * (near * step), modulus, inverse, scale)
    for index in range(FINE // near):
        here = tuple(part[index : index + 1] for part in high)
        cosine, sine = combine(here, low)
        table_ref[near * index : near * (index + 1), :slots] = cosine.astype(jnp.bfloat16)
        table_ref[near * index : near * (index + 1), slots:] = sine.astype(jnp.bfloat16)
    step = lax.broadcasted_iota(jnp.int32, (8, slots), 0)
    low = turn(twice * (FINE * step) + orders * offset, modulus, inverse, scale)
    high = turn(twice * (8 * FINE * step), modulus, inverse, scale)
    for index in range(coarse // 8):
        here = tuple(part[index : index + 1] for part in high)
        cosine, sine = combine(here, low)
        outer_ref[8 * index : 8 * (index + 1), :slots] = cosine
        outer_ref[8 * index : 8 * (index + 1), slots:] = sine
    pixels = lax.broadcasted_iota(jnp.int32, (1, pixel_slots), 1)
    mask = jnp.where(pixels < count, mask_ref[...], 0.0)
    square = jnp.sum(mask * mask)
    table = table_ref[...]
    real_sum = jnp.zeros((rows, slots), jnp.float32)
    imag_sum = jnp.zeros((rows, slots), jnp.float32)
    for group in range(coarse // GROUP):
        buffer = rows_ref.at[group % 2]
        for member in range(GROUP):
            first = (group * GROUP + member) * FINE
            block = maps_ref[:, first : first + FINE].astype(jnp.float32) * mask[:, first : first + FINE]
            buffer[member * rows : (member + 1) * rows, :] = block.astype(jnp.bfloat16)
        inner = jnp.dot(buffer[...], table, preferred_element_type=jnp.float32)
        for member in range(GROUP):
            index = group * GROUP + member
            cosine = outer_ref[index : index + 1, :slots]
            sine = outer_ref[index : index + 1, slots:]
            inner_cos = inner[member * rows : (member + 1) * rows, :slots]
            inner_sin = inner[member * rows : (member + 1) * rows, slots:]
            real_sum = real_sum + (cosine * inner_cos - sine * inner_sin)
            imag_sum = imag_sum + (sine * inner_cos + cosine * inner_sin)
    inverse_root = 1.0 / jnp.sqrt(count_float)
    live = twice < count
    real_part = jnp.where(live, real_sum * inverse_root, 0.0)
    imag_part = jnp.where(live, -imag_sum * inverse_root, 0.0)
    joined = jnp.concatenate(
        [real_part[:maps_count], imag_part[:maps_count], real_part[maps_count:], imag_part[maps_count:]], axis=0
    )
    half = slots // 2
    coef_ref[0] = jnp.transpose(joined[:, :half]).astype(jnp.bfloat16)
    coef_ref[1] = jnp.transpose(joined[:, half:]).astype(jnp.bfloat16)
    lane = lax.broadcasted_iota(jnp.int32, sums_ref.shape, 1)
    value = jnp.where(lane < 3, square, count_float)
    top = value.astype(jnp.bfloat16).astype(jnp.float32)
    middle = (value - top).astype(jnp.bfloat16).astype(jnp.float32)
    bottom = ((value - top) - middle).astype(jnp.bfloat16).astype(jnp.float32)
    kind = lane % 3
    pieces = jnp.where(kind == 0, top, jnp.where(kind == 1, middle, bottom))
    sums_ref[...] = jnp.where(lane < 6, pieces, 0.0).astype(jnp.bfloat16)


def fourier(maps, mask, count, offset, orders):
    rows, pixel_slots = maps.shape
    slots = orders.shape[1]
    return pl.pallas_call(
        fourier_kernel,
        out_shape=(
            jax.ShapeDtypeStruct((2, slots // 2, 2 * rows), jnp.bfloat16),
            jax.ShapeDtypeStruct((1, 2 * rows), jnp.bfloat16),
        ),
        in_specs=[SMEM_SPEC, SMEM_SPEC, VMEM_SPEC, VMEM_SPEC, VMEM_SPEC],
        out_specs=(VMEM_SPEC, VMEM_SPEC),
        scratch_shapes=[
            pltpu.VMEM((FINE, 2 * slots), jnp.bfloat16),
            pltpu.VMEM((pixel_slots // FINE, 2 * slots), jnp.float32),
            pltpu.VMEM((2, GROUP * rows, FINE), jnp.bfloat16),
        ],
        name="fourier",
    )(count, offset, orders, mask, maps)


def reversed_rows(block):
    rows = block.shape[0]
    index = 7 - lax.broadcasted_iota(jnp.int32, (8, block.shape[1]), 0)
    tiles = [
        jnp.take_along_axis(block[8 * t : 8 * (t + 1)], index, axis=0) for t in range(rows // 8)
    ]
    return jnp.concatenate(tiles[::-1], axis=0)


def alm_kernel(order_ref, coef_ref, legendre_ref, alm_ref, send_ref, operand_ref, held_ref):
    tile = pl.program_id(0)
    tiles = pl.num_programs(0)
    height = legendre_ref.shape[0]
    columns = coef_ref.shape[2]
    quarter = columns // 4
    degrees = held_ref.shape[0] - 64
    order = order_ref[0]
    split = degrees - order

    @pl.when(tile == 0)
    def _():
        row = lax.broadcasted_iota(jnp.int32, (columns, columns), 0)
        column = lax.broadcasted_iota(jnp.int32, (columns, columns), 1)
        part = column // quarter
        hit = (row // quarter == 3 - part) & (row % quarter == column % quarter)
        sign = jnp.where((part == 1) | (part == 2), -1.0, 1.0)
        swap = jnp.where(hit, sign, 0.0).astype(jnp.bfloat16)
        for slot in range(2):
            block = coef_ref[slot]
            lower = jnp.dot(block, swap, preferred_element_type=jnp.float32)
            operand_ref[slot, : block.shape[0]] = -block
            operand_ref[slot, block.shape[0] :] = (-lower).astype(jnp.bfloat16)

    first_row = tile * height
    rows = legendre_ref[...]
    slot = (first_row >= split).astype(jnp.int32)
    product = jnp.dot(rows, operand_ref[slot], preferred_element_type=jnp.float32)
    alm_ref[...] = product
    held_ref[pl.ds(32 + pl.multiple_of(first_row, height), height)] = product

    @pl.when((first_row < split) & (split < first_row + height))
    def _():
        other = jnp.dot(rows, operand_ref[1], preferred_element_type=jnp.float32)
        row_index = first_row + lax.broadcasted_iota(jnp.int32, (height, 1), 0)
        fixed = jnp.where(row_index >= split, other, product)
        alm_ref[...] = fixed
        held_ref[pl.ds(32 + pl.multiple_of(first_row, height), height)] = fixed

    @pl.when(tile == tiles - 1)
    def _():
        devices = send_ref.shape[0] // 64
        step = lax.broadcasted_iota(jnp.int32, (32, 1), 0)

        def one(device, carry):
            upper = device >= devices // 2
            block = jnp.where(upper, devices - 1 - device, device)
            low = 64 * block + 32 * upper.astype(jnp.int32)
            kept = held_ref[pl.ds(32 + jnp.maximum(low - order, -32), 32)]
            moved = reversed_rows(held_ref[pl.ds(pl.multiple_of(degrees - low, 32), 32)])
            mirror = reversed_rows(held_ref[pl.ds(degrees - low - order, 32)])
            start = pl.multiple_of(device * 64, 64)
            send_ref[pl.ds(start, 32)] = jnp.where(step >= order - low, kept, moved).astype(jnp.bfloat16)
            send_ref[pl.ds(start + 32, 32)] = mirror.astype(jnp.bfloat16)
            return carry

        lax.fori_loop(0, devices, one, 0, unroll=2)


def alm_and_send(order, coef, legendre, height=512):
    degrees, inner = legendre.shape
    columns = coef.shape[2]
    return pl.pallas_call(
        alm_kernel,
        grid=(degrees // height,),
        out_shape=(
            jax.ShapeDtypeStruct((degrees, columns), jnp.float32),
            jax.ShapeDtypeStruct((degrees, columns), jnp.bfloat16),
        ),
        in_specs=[
            SMEM_SPEC,
            VMEM_SPEC,
            pl.BlockSpec((height, inner), lambda t: (t, 0)),
        ],
        out_specs=(pl.BlockSpec((height, columns), lambda t: (t, 0)), VMEM_SPEC),
        scratch_shapes=[
            pltpu.VMEM((2, inner, columns), jnp.bfloat16),
            pltpu.VMEM((degrees + 64, columns), jnp.float32),
        ],
        compiler_params=pltpu.CompilerParams(dimension_semantics=("arbitrary",)),
        name="alm_and_send",
    )(order, coef, legendre)


def outer_totals(rows, maps_count):
    split_parts = rows.reshape(rows.shape[0], rows.shape[1], 2, 2, maps_count)
    return jnp.einsum(
        "slerm,slern->lemn", split_parts, split_parts, preferred_element_type=jnp.float32
    )


def scaled_spectra(totals, degrees, orders, weight, maps_count):
    counts = jnp.maximum(
        jnp.sum((orders[None, :] <= degrees[:, None]).astype(jnp.int32), axis=1), 1
    ).astype(jnp.float32)
    return (2.0 * totals / (weight * counts)[:, None, None, None]).reshape(
        degrees.shape[0], 2, maps_count * maps_count
    )


def local(sky_maps, sky_mask, pixel_counts, phi_offsets, low_orders, legendre):
    devices = lax.axis_size(BAND_SUB)
    device_index = lax.axis_index(BAND_SUB)
    degree_count = legendre.shape[1]
    maps_count = sky_maps.shape[2]
    columns = 4 * maps_count
    orders = jnp.concatenate([low_orders, degree_count - low_orders])
    coef, sums = fourier(
        sky_maps.reshape(2 * maps_count, sky_maps.shape[3]), sky_mask, pixel_counts, phi_offsets, orders[None]
    )
    outgoing = jnp.concatenate(
        [jnp.swapaxes(coef, 0, 1), jnp.broadcast_to(sums[:, None], (devices, 2, columns))], axis=1
    )
    received = lax.all_to_all(outgoing, BAND_SUB, split_axis=0, concat_axis=0, tiled=True)
    blocks = jnp.swapaxes(received[:, :2], 0, 1)
    pieces = received[:, 2, :6].astype(jnp.float32)
    totals = jnp.sum(pieces.reshape(devices, 2, 3).sum(axis=2), axis=0)
    weight = totals[0] / totals[1]
    order = lax.dynamic_slice_in_dim(low_orders, device_index, 1, 0)
    alm, send = alm_and_send(order, blocks, legendre[0])
    range_rows = degree_count // devices
    half_rows = range_rows // 2
    incoming = lax.all_to_all(
        send.reshape(devices, range_rows, columns), BAND_SUB, split_axis=0, concat_axis=0, tiled=True
    )
    upper_device = device_index >= devices // 2
    pair_block = jnp.minimum(device_index, devices - 1 - device_index)
    own_low = (
        pair_block * range_rows
        + upper_device.astype(jnp.int32) * half_rows
        + jnp.arange(half_rows, dtype=jnp.int32)
    )
    own_mirror = degree_count - 1 - own_low
    kept_mask = own_low[None, :] >= low_orders[:, None]
    low_rows = incoming[:, :half_rows]
    mirror_rows = incoming[:, half_rows:]
    low_kept = jnp.where(kept_mask[:, :, None], low_rows, jnp.zeros_like(low_rows))
    low_moved = jnp.where(kept_mask[:, :, None], jnp.zeros_like(low_rows), low_rows)
    low_totals = outer_totals(low_kept, maps_count)
    mirror_totals = outer_totals(mirror_rows, maps_count) + outer_totals(low_moved, maps_count)
    low_spectra = scaled_spectra(low_totals, own_low, orders, weight, maps_count)
    mirror_spectra = jnp.flip(
        scaled_spectra(mirror_totals, own_mirror, orders, weight, maps_count), axis=0
    )
    swapped = jnp.where(upper_device, low_spectra, mirror_spectra)
    route = [(device, devices - 1 - device) for device in range(devices)]
    swapped = lax.ppermute(swapped.astype(jnp.bfloat16), BAND_SUB, route).astype(jnp.float32)
    spectra = jnp.where(
        upper_device,
        jnp.concatenate([mirror_spectra, swapped], axis=0),
        jnp.concatenate([low_spectra, swapped], axis=0),
    )
    return (alm[None], spectra)


def solution(mesh):
    torus = Mesh(
        mesh.devices.reshape(mesh.shape["groups"], 8, 8, mesh.shape["sub"]),
        ("groups", "band_0", "band_1", "sub"),
    )
    in_specs = (
        P(GROUPS_BAND_SUB, None, None, None),
        P(GROUPS_BAND_SUB, None),
        P(GROUPS_BAND_SUB),
        P(GROUPS_BAND_SUB),
        P("groups"),
        P(GROUPS_BAND_SUB, None, None),
    )
    out_specs = (P(GROUPS_BAND_SUB, None, None), P(GROUPS_BAND_SUB, None, None))
    return jax.shard_map(local, mesh=torus, in_specs=in_specs, out_specs=out_specs, check_vma=False)
```

```python
import functools

import jax
import jax.numpy as jnp
from jax import lax
from jax.experimental import pallas as pl
from jax.experimental.pallas import tpu as pltpu
from jax.sharding import Mesh
from jax.sharding import PartitionSpec as P

BAND_SUB = ("band_0", "band_1", "sub")
GROUPS_BAND_SUB = ("groups", "band_0", "band_1", "sub")
CHUNKS = 1

FINE = 256
GROUP = 8
PITCH = 132
VMEM_SPEC = pl.BlockSpec(memory_space=pltpu.VMEM)
SMEM_SPEC = pl.BlockSpec(memory_space=pltpu.SMEM)
ANY_SPEC = pl.BlockSpec(memory_space=pl.ANY)


def mod_units(units, modulus, inverse):
    quotient = jnp.floor(units.astype(jnp.float32) * inverse).astype(jnp.int32)
    rest = units - quotient * modulus
    rest = jnp.where(rest < 0, rest + modulus, rest)
    return jnp.where(rest >= modulus, rest - modulus, rest)


def turn(units, modulus, inverse, scale):
    angle = scale * mod_units(units, modulus, inverse).astype(jnp.float32)
    return jnp.cos(angle), jnp.sin(angle)


def combine(first, second):
    (a_cos, a_sin), (b_cos, b_sin) = first, second
    return a_cos * b_cos - a_sin * b_sin, a_sin * b_cos + a_cos * b_sin


def fourier_kernel(
    degrees, count_ref, offset_ref, order_ref, mask_ref, maps_ref, out_ref, table_ref, outer_ref, rows_ref, join_ref
):
    pixel_slots = maps_ref.shape[1]
    rows = maps_ref.shape[0]
    maps_count = rows // 2
    pairs = order_ref.shape[1]
    slots = 2 * pairs
    count = count_ref[0]
    offset = offset_ref[0]
    count_float = count.astype(jnp.float32)
    modulus = 2 * count
    inverse = 1.0 / modulus.astype(jnp.float32)
    scale = jnp.pi / count_float
    low_orders = order_ref[...]
    orders = jnp.concatenate([low_orders, degrees - low_orders], axis=1)
    twice = 2 * orders
    coarse = pixel_slots // FINE
    near = 16
    step = lax.broadcasted_iota(jnp.int32, (near, slots), 0)
    low = turn(twice * step, modulus, inverse, scale)
    high = turn(twice * (near * step), modulus, inverse, scale)
    for index in range(FINE // near):
        here = tuple(part[index : index + 1] for part in high)
        cosine, sine = combine(here, low)
        table_ref[near * index : near * (index + 1), :slots] = cosine.astype(jnp.bfloat16)
        table_ref[near * index : near * (index + 1), slots:] = sine.astype(jnp.bfloat16)
    step = lax.broadcasted_iota(jnp.int32, (8, slots), 0)
    low = turn(twice * (FINE * step) + orders * offset, modulus, inverse, scale)
    high = turn(twice * (8 * FINE * step), modulus, inverse, scale)
    for index in range(coarse // 8):
        here = tuple(part[index : index + 1] for part in high)
        cosine, sine = combine(here, low)
        outer_ref[8 * index : 8 * (index + 1), :slots] = cosine
        outer_ref[8 * index : 8 * (index + 1), slots:] = sine
    pixels = lax.broadcasted_iota(jnp.int32, (1, pixel_slots), 1)
    mask = jnp.where(pixels < count, mask_ref[...], 0.0)
    square = jnp.sum(mask * mask)
    table = table_ref[...]
    real_sum = jnp.zeros((rows, slots), jnp.float32)
    imag_sum = jnp.zeros((rows, slots), jnp.float32)
    for group in range(coarse // GROUP):
        buffer = rows_ref.at[group % 2]
        for member in range(GROUP):
            first = (group * GROUP + member) * FINE
            block = maps_ref[:, first : first + FINE].astype(jnp.float32) * mask[:, first : first + FINE]
            buffer[member * rows : (member + 1) * rows, :] = block.astype(jnp.bfloat16)
        inner = jnp.dot(buffer[...], table, preferred_element_type=jnp.float32)
        for member in range(GROUP):
            index = group * GROUP + member
            cosine = outer_ref[index : index + 1, :slots]
            sine = outer_ref[index : index + 1, slots:]
            inner_cos = inner[member * rows : (member + 1) * rows, :slots]
            inner_sin = inner[member * rows : (member + 1) * rows, slots:]
            real_sum = real_sum + (cosine * inner_cos - sine * inner_sin)
            imag_sum = imag_sum + (sine * inner_cos + cosine * inner_sin)
    inverse_root = 1.0 / jnp.sqrt(count_float)
    live = twice < count
    real_part = jnp.where(live, real_sum * inverse_root, 0.0)
    imag_part = jnp.where(live, -imag_sum * inverse_root, 0.0)
    joined = jnp.concatenate(
        [real_part[:maps_count], imag_part[:maps_count], real_part[maps_count:], imag_part[maps_count:]], axis=0
    )
    join_ref[pl.ds(0, pairs, stride=4)] = jnp.transpose(joined[:, :pairs])
    join_ref[pl.ds(1, pairs, stride=4)] = jnp.transpose(joined[:, pairs:])
    lane = lax.broadcasted_iota(jnp.int32, (1, 2 * rows), 1)
    value = jnp.where(lane < 3, square, count_float)
    top = value.astype(jnp.bfloat16).astype(jnp.float32)
    middle = (value - top).astype(jnp.bfloat16).astype(jnp.float32)
    bottom = ((value - top) - middle).astype(jnp.bfloat16).astype(jnp.float32)
    kind = lane % 3
    pieces = jnp.where(kind == 0, top, jnp.where(kind == 1, middle, bottom))
    pieces = jnp.broadcast_to(jnp.where(lane < 6, pieces, 0.0), (pairs, 2 * rows))
    join_ref[pl.ds(2, pairs, stride=4)] = pieces
    join_ref[pl.ds(3, pairs, stride=4)] = pieces
    out_ref[...] = join_ref[...].astype(jnp.bfloat16)


def fourier(maps, mask, count, offset, low_orders, degrees):
    rows, pixel_slots = maps.shape
    pairs = low_orders.shape[1]
    slots = 2 * pairs
    return pl.pallas_call(
        functools.partial(fourier_kernel, degrees),
        out_shape=jax.ShapeDtypeStruct((4 * pairs, 2 * rows), jnp.bfloat16),
        in_specs=[SMEM_SPEC, SMEM_SPEC, VMEM_SPEC, VMEM_SPEC, VMEM_SPEC],
        out_specs=VMEM_SPEC,
        scratch_shapes=[
            pltpu.VMEM((FINE, 2 * slots), jnp.bfloat16),
            pltpu.VMEM((pixel_slots // FINE, 2 * slots), jnp.float32),
            pltpu.VMEM((2, GROUP * rows, FINE), jnp.bfloat16),
            pltpu.VMEM((4 * pairs, 2 * rows), jnp.float32),
        ],
        name="fourier",
    )(count, offset, low_orders, mask, maps)


def alm_kernel(
    chunks, height, order_ref, given_ref, legendre_ref, alm_ref, weight_ref, *rest
):
    send_refs = rest[:chunks]
    given32_ref, operand_ref, held_ref, sem = rest[chunks:]
    columns = given_ref.shape[1]
    cycles = given_ref.shape[0] // 4
    quarter = columns // 4
    degrees = legendre_ref.shape[0]
    order = order_ref[0]
    split = degrees - order
    given32_ref[...] = given_ref[...].astype(jnp.float32)
    row = lax.broadcasted_iota(jnp.int32, (columns, columns), 0)
    column = lax.broadcasted_iota(jnp.int32, (columns, columns), 1)
    part = column // quarter
    hit = (row // quarter == 3 - part) & (row % quarter == column % quarter)
    sign = jnp.where((part == 1) | (part == 2), -1.0, 1.0)
    swap = jnp.where(hit, sign, 0.0).astype(jnp.bfloat16)
    for slot in range(2):
        block = given32_ref[pl.ds(slot, cycles, stride=4)].astype(jnp.bfloat16)
        lower = jnp.dot(block, swap, preferred_element_type=jnp.float32)
        operand_ref[slot, :cycles] = -block
        operand_ref[slot, cycles:] = (-lower).astype(jnp.bfloat16)

    for tile in range(degrees // height):
        first_row = tile * height
        rows = legendre_ref[first_row : first_row + height]
        slot = (first_row >= split).astype(jnp.int32)
        held_ref[32 + first_row : 32 + first_row + height] = jnp.dot(
            rows, operand_ref[slot], preferred_element_type=jnp.float32
        )
    border = pl.multiple_of(split // height * height, height)
    other = jnp.dot(legendre_ref[pl.ds(border, height)], operand_ref[1], preferred_element_type=jnp.float32)
    row_index = border + lax.broadcasted_iota(jnp.int32, (height, 1), 0)
    place = pl.ds(32 + border, height)
    held_ref[place] = jnp.where(row_index >= split, other, held_ref[place])
    copy = pltpu.make_async_copy(held_ref.at[pl.ds(32, degrees)], alm_ref, sem)
    copy.start()

    pieces = given32_ref[pl.ds(2, cycles, stride=4)]
    lane = lax.broadcasted_iota(jnp.int32, pieces.shape, 1)
    square = jnp.sum(jnp.where(lane < 3, pieces, 0.0))
    pixels = jnp.sum(jnp.where(lane < 3, 0.0, pieces))
    weight_ref[...] = jnp.full(weight_ref.shape, square / pixels, jnp.float32)

    half = send_refs[0].shape[0] // cycles // 2
    step = lax.broadcasted_iota(jnp.int32, (half, 1), 0)

    def one(device, carry):
        upper = device >= cycles // 2
        block = jnp.where(upper, cycles - 1 - device, device)
        start = pl.multiple_of(device * 2 * half, 2 * half)
        for chunk in range(chunks):
            low = 2 * chunks * half * block + chunks * half * upper.astype(jnp.int32) + chunk * half
            kept = held_ref[pl.ds(32 + jnp.maximum(low - order, -half), half)]
            moved = held_ref[pl.ds(32 + degrees - jnp.minimum(low + half, order), half)]
            mirror = held_ref[pl.ds(32 + degrees - half - low - order, half)]
            mixed = jnp.where(step >= order - low, kept, moved)
            send_refs[chunk][pl.ds(start, half)] = mixed.astype(jnp.bfloat16)
            send_refs[chunk][pl.ds(start + half, half)] = mirror.astype(jnp.bfloat16)
        return carry

    lax.fori_loop(0, cycles, one, 0, unroll=4)
    copy.wait()


def alm_and_send(order, given, legendre, chunks, height=512):
    degrees, inner = legendre.shape
    columns = given.shape[1]
    send = jax.ShapeDtypeStruct((degrees // chunks, columns), jnp.bfloat16)
    return pl.pallas_call(
        functools.partial(alm_kernel, chunks, height),
        out_shape=(
            jax.ShapeDtypeStruct((degrees, columns), jnp.float32),
            jax.ShapeDtypeStruct((1, columns), jnp.float32),
        )
        + (send,) * chunks,
        in_specs=[SMEM_SPEC, VMEM_SPEC, VMEM_SPEC],
        out_specs=(ANY_SPEC, VMEM_SPEC) + (VMEM_SPEC,) * chunks,
        scratch_shapes=[
            pltpu.VMEM(given.shape, jnp.float32),
            pltpu.VMEM((2, inner, columns), jnp.bfloat16),
            pltpu.VMEM((degrees + 64, columns), jnp.float32),
            pltpu.SemaphoreType.DMA,
        ],
        name="alm_and_send",
    )(order, given, legendre)


def spectra_kernel(
    chunk, degrees, start_ref, order_ref, order_row_ref, weight_ref, rows_ref, low_ref, mirror_ref,
    kept_ref, moved_ref, mirrored_ref, gram_ref, factor_ref,
):
    pairs = order_row_ref.shape[1]
    half = rows_ref.shape[0] // pairs // 2
    first = start_ref[0] + chunk * half
    step = lax.broadcasted_iota(jnp.int32, (half, 1), 0)
    columns = rows_ref.shape[1]
    quarter = columns // 4
    moved_ref[0 : half * PITCH] = jnp.zeros((half * PITCH, columns), jnp.float32)

    def one(pair, carry):
        start = pl.multiple_of(pair * 2 * half, 2 * half)
        block = rows_ref[pl.ds(start, 2 * half)].astype(jnp.float32)
        order = order_ref[pair]
        early = jnp.clip(order - first, 0, half)
        kept_ref[pl.ds(pair, half, stride=PITCH)] = jnp.where(step >= early, block[:half], 0.0)
        moved_ref[pl.ds((half - early) * PITCH + pair, half, stride=PITCH)] = block[:half]
        mirrored_ref[pl.ds(pair, half, stride=PITCH)] = block[half:]
        return carry

    lax.fori_loop(0, pairs, one, 0, unroll=4)

    orders = order_row_ref[...]
    weight = weight_ref[...]
    low_degree = first + step
    mirror_degree = degrees - half - first + step
    for kind, degree in enumerate((low_degree, mirror_degree)):
        below = (orders <= degree).astype(jnp.float32) + (degrees - orders <= degree).astype(jnp.float32)
        counts = jnp.maximum(jnp.sum(below, axis=1, keepdims=True), 1.0)
        factor_ref[kind * half : (kind + 1) * half] = 2.0 / (weight * counts)

    def gram(rows):
        return lax.dot_general(rows, rows, (((0,), (0,)), ((), ())), preferred_element_type=jnp.float32)

    lane_group = lax.broadcasted_iota(jnp.int32, (8, columns), 1) // quarter

    def flat(total, slot, out_ref, index, factor):
        for part in range(2):
            base = 2 * part * quarter
            real = total[base : base + quarter]
            imag = total[base + quarter : base + 2 * quarter]
            gram_ref[2 * slot + part] = real + pltpu.roll(imag, columns - quarter, 1)
            row = None
            for member in range(4):
                piece = gram_ref[2 * slot + part, pl.ds(member, 8, stride=4)]
                shift = (member * quarter - base) % columns
                if shift:
                    piece = pltpu.roll(piece, shift, 1)
                row = piece if row is None else jnp.where(lane_group == member, piece, row)
            out_ref[pl.ds(index * 16 + part, 8, stride=2)] = row * factor

    def degree_step(index, carry):
        place = pl.ds(index * PITCH, pairs)
        total = gram(kept_ref[place].astype(jnp.bfloat16))
        flat(total, 0, low_ref, index, factor_ref[pl.ds(index, 1)])
        total = gram(moved_ref[place].astype(jnp.bfloat16)) + gram(mirrored_ref[place].astype(jnp.bfloat16))
        flat(total, 1, mirror_ref, index, factor_ref[pl.ds(half + index, 1)])
        return carry

    lax.fori_loop(0, half, degree_step, 0, unroll=2)


def spectra_rows(start, low_orders, weight, rows, chunk, chunks, degrees):
    pairs = low_orders.shape[0]
    columns = rows.shape[1]
    half = rows.shape[0] // pairs // 2
    out = jax.ShapeDtypeStruct((half * 16, columns), jnp.float32)
    return pl.pallas_call(
        functools.partial(spectra_kernel, chunk, degrees),
        out_shape=(out, out),
        in_specs=[SMEM_SPEC, SMEM_SPEC, VMEM_SPEC, VMEM_SPEC, VMEM_SPEC],
        out_specs=(VMEM_SPEC, VMEM_SPEC),
        scratch_shapes=[
            pltpu.VMEM((half * PITCH, columns), jnp.float32),
            pltpu.VMEM((2 * half * PITCH, columns), jnp.float32),
            pltpu.VMEM((half * PITCH, columns), jnp.float32),
            pltpu.VMEM((4, 32, columns), jnp.float32),
            pltpu.VMEM((2 * half, columns), jnp.float32),
        ],
        name=f"spectra_{chunk}",
    )(start, low_orders, low_orders[None], weight, rows)


def in_degree_order(rows, columns):
    tiles = rows.reshape(-1, 8, 2, columns)
    return jnp.swapaxes(tiles, 1, 2).reshape(-1, 2, 8 * columns)


def local(sky_maps, sky_mask, pixel_counts, phi_offsets, low_orders, legendre):
    devices = lax.axis_size(BAND_SUB)
    device_index = lax.axis_index(BAND_SUB)
    degree_count = legendre.shape[1]
    rows = sky_maps.shape[1] * sky_maps.shape[2]
    columns = 2 * rows
    range_rows = degree_count // devices
    outgoing = fourier(
        sky_maps.reshape(rows, sky_maps.shape[3]), sky_mask, pixel_counts, phi_offsets, low_orders[None], degree_count
    )
    received = lax.all_to_all(
        outgoing.reshape(devices, 4, columns), BAND_SUB, split_axis=0, concat_axis=0, tiled=True
    )
    order = lax.dynamic_slice_in_dim(low_orders, device_index, 1, 0)
    alm, weight, *sends = alm_and_send(order, received.reshape(4 * devices, columns), legendre[0], CHUNKS)
    upper_device = device_index >= devices // 2
    pair_block = jnp.minimum(device_index, devices - 1 - device_index)
    start = pair_block * range_rows + upper_device.astype(jnp.int32) * (range_rows // 2)
    route = [(device, devices - 1 - device) for device in range(devices)]
    kept, swapped = [], []
    for chunk, send in enumerate(sends):
        incoming = lax.all_to_all(
            send.reshape(devices, -1, columns), BAND_SUB, split_axis=0, concat_axis=0, tiled=True
        )
        low, mirror = spectra_rows(
            start[None], low_orders, weight, incoming.reshape(-1, columns), chunk, CHUNKS, degree_count
        )
        kept.append(jnp.where(upper_device, mirror, low))
        moving = jnp.where(upper_device, low, mirror).astype(jnp.bfloat16)
        swapped.append(lax.ppermute(moving, BAND_SUB, route).astype(jnp.float32))
    spectra = jnp.concatenate(kept + swapped, axis=0)
    return (alm[None], in_degree_order(spectra, columns))


def solution(mesh):
    torus = Mesh(
        mesh.devices.reshape(mesh.shape["groups"], 8, 8, mesh.shape["sub"]),
        ("groups", "band_0", "band_1", "sub"),
    )
    in_specs = (
        P(GROUPS_BAND_SUB, None, None, None),
        P(GROUPS_BAND_SUB, None),
        P(GROUPS_BAND_SUB),
        P(GROUPS_BAND_SUB),
        P("groups"),
        P(GROUPS_BAND_SUB, None, None),
    )
    out_specs = (P(GROUPS_BAND_SUB, None, None), P(GROUPS_BAND_SUB, None, None))
    return jax.shard_map(local, mesh=torus, in_specs=in_specs, out_specs=out_specs, check_vma=False)
```

```python
import functools

import jax
import jax.numpy as jnp
from jax import lax
from jax.experimental import pallas as pl
from jax.experimental.pallas import tpu as pltpu
from jax.sharding import Mesh
from jax.sharding import PartitionSpec as P

BAND_SUB = ("band_0", "band_1", "sub")
GROUPS_BAND_SUB = ("groups", "band_0", "band_1", "sub")

FINE = 256
GROUP = 8
PITCH = 132
READS = 2
PIECES = 2
MAP_READS = 2
SLOTS = 16
GRAMS = 16
PARTS = 4
UNROLL = 4
VMEM_LIMIT = 67043328
VMEM_SPEC = pl.BlockSpec(memory_space=pltpu.VMEM)
SMEM_SPEC = pl.BlockSpec(memory_space=pltpu.SMEM)
HBM_SPEC = pl.BlockSpec(memory_space=pltpu.HBM)


def mod_units(units, modulus, inverse):
    quotient = jnp.floor(units.astype(jnp.float32) * inverse).astype(jnp.int32)
    rest = units - quotient * modulus
    rest = jnp.where(rest < 0, rest + modulus, rest)
    return jnp.where(rest >= modulus, rest - modulus, rest)


def turn(units, modulus, inverse, scale):
    angle = scale * mod_units(units, modulus, inverse).astype(jnp.float32)
    return jnp.cos(angle), jnp.sin(angle)


def combine(first, second):
    (a_cos, a_sin), (b_cos, b_sin) = first, second
    return a_cos * b_cos - a_sin * b_sin, a_sin * b_cos + a_cos * b_sin


def fourier_kernel(
    degrees, count_ref, offset_ref, order_hbm, mask_hbm, maps_hbm, out_ref, table_ref, outer_ref, rows_ref, join_ref,
    maps_ref, sems, order_ref, mask_ref, small_sems,
):
    small = [
        pltpu.make_async_copy(source, target, small_sems.at[index])
        for index, (source, target) in enumerate(((order_hbm, order_ref), (mask_hbm, mask_ref)))
    ]
    for copy in small:
        copy.start()
    width = maps_hbm.shape[1] // sems.shape[0]
    copies = []
    for group in range(sems.shape[0]):
        place = pl.ds(group * width, width)
        copy = pltpu.make_async_copy(maps_hbm.at[:, place], maps_ref.at[:, place], sems.at[group])
        copy.start()
        copies.append(copy)
    pixel_slots = maps_ref.shape[1]
    rows = maps_ref.shape[0]
    maps_count = rows // 2
    pairs = order_ref.shape[1]
    slots = 2 * pairs
    for copy in small:
        copy.wait()
    count = count_ref[0]
    offset = offset_ref[0]
    count_float = count.astype(jnp.float32)
    modulus = 2 * count
    inverse = 1.0 / modulus.astype(jnp.float32)
    scale = jnp.pi / count_float
    low_orders = order_ref[...]
    orders = jnp.concatenate([low_orders, degrees - low_orders], axis=1)
    twice = 2 * orders
    coarse = pixel_slots // FINE
    near = 16
    step = lax.broadcasted_iota(jnp.int32, (near, slots), 0)
    low = turn(twice * step, modulus, inverse, scale)
    high = turn(twice * (near * step), modulus, inverse, scale)
    for index in range(FINE // near):
        here = tuple(part[index : index + 1] for part in high)
        cosine, sine = combine(here, low)
        table_ref[near * index : near * (index + 1), :slots] = cosine.astype(jnp.bfloat16)
        table_ref[near * index : near * (index + 1), slots:] = sine.astype(jnp.bfloat16)
    step = lax.broadcasted_iota(jnp.int32, (8, slots), 0)
    low = turn(twice * (FINE * step) + orders * offset, modulus, inverse, scale)
    high = turn(twice * (8 * FINE * step), modulus, inverse, scale)
    for index in range(coarse // 8):
        here = tuple(part[index : index + 1] for part in high)
        cosine, sine = combine(here, low)
        outer_ref[8 * index : 8 * (index + 1), :slots] = cosine
        outer_ref[8 * index : 8 * (index + 1), slots:] = sine
    pixels = lax.broadcasted_iota(jnp.int32, (1, pixel_slots), 1)
    mask = jnp.where(pixels < count, mask_ref[...], 0.0)
    square = jnp.sum(mask * mask)
    table = table_ref[...]
    real_sum = jnp.zeros((rows, slots), jnp.float32)
    imag_sum = jnp.zeros((rows, slots), jnp.float32)
    for group in range(coarse // GROUP):
        if group * GROUP * FINE % width == 0:
            copies[group * GROUP * FINE // width].wait()
        buffer = rows_ref.at[group % 2]
        for member in range(GROUP):
            first = (group * GROUP + member) * FINE
            block = maps_ref[:, first : first + FINE].astype(jnp.float32) * mask[:, first : first + FINE]
            buffer[member * rows : (member + 1) * rows, :] = block.astype(jnp.bfloat16)
        inner = jnp.dot(buffer[...], table, preferred_element_type=jnp.float32)
        for member in range(GROUP):
            index = group * GROUP + member
            cosine = outer_ref[index : index + 1, :slots]
            sine = outer_ref[index : index + 1, slots:]
            inner_cos = inner[member * rows : (member + 1) * rows, :slots]
            inner_sin = inner[member * rows : (member + 1) * rows, slots:]
            real_sum = real_sum + (cosine * inner_cos - sine * inner_sin)
            imag_sum = imag_sum + (sine * inner_cos + cosine * inner_sin)
    inverse_root = 1.0 / jnp.sqrt(count_float)
    live = twice < count
    real_part = jnp.where(live, real_sum * inverse_root, 0.0)
    imag_part = jnp.where(live, -imag_sum * inverse_root, 0.0)
    joined = jnp.concatenate(
        [real_part[:maps_count], imag_part[:maps_count], real_part[maps_count:], imag_part[maps_count:]], axis=0
    )
    join_ref[pl.ds(0, pairs, stride=4)] = jnp.transpose(joined[:, :pairs])
    join_ref[pl.ds(1, pairs, stride=4)] = jnp.transpose(joined[:, pairs:])
    lane = lax.broadcasted_iota(jnp.int32, (1, 2 * rows), 1)
    value = jnp.where(lane < 3, square, count_float)
    top = value.astype(jnp.bfloat16).astype(jnp.float32)
    middle = (value - top).astype(jnp.bfloat16).astype(jnp.float32)
    bottom = ((value - top) - middle).astype(jnp.bfloat16).astype(jnp.float32)
    kind = lane % 3
    pieces = jnp.where(kind == 0, top, jnp.where(kind == 1, middle, bottom))
    pieces = jnp.broadcast_to(jnp.where(lane < 6, pieces, 0.0), (pairs, 2 * rows))
    join_ref[pl.ds(2, pairs, stride=4)] = pieces
    join_ref[pl.ds(3, pairs, stride=4)] = pieces
    out_ref[...] = join_ref[...].astype(jnp.bfloat16)


def fourier(maps, mask, count, offset, low_orders, degrees):
    rows, pixel_slots = maps.shape
    pairs = low_orders.shape[1]
    slots = 2 * pairs
    return pl.pallas_call(
        functools.partial(fourier_kernel, degrees),
        out_shape=jax.ShapeDtypeStruct((4 * pairs, 2 * rows), jnp.bfloat16),
        in_specs=[SMEM_SPEC] * 2 + [HBM_SPEC] * 3,
        out_specs=VMEM_SPEC,
        scratch_shapes=[
            pltpu.VMEM((FINE, 2 * slots), jnp.bfloat16),
            pltpu.VMEM((pixel_slots // FINE, 2 * slots), jnp.float32),
            pltpu.VMEM((2, GROUP * rows, FINE), jnp.bfloat16),
            pltpu.VMEM((4 * pairs, 2 * rows), jnp.float32),
            pltpu.VMEM((rows, pixel_slots), jnp.bfloat16),
            pltpu.SemaphoreType.DMA((MAP_READS,)),
            pltpu.VMEM((1, pairs), jnp.int32),
            pltpu.VMEM((1, pixel_slots), jnp.float32),
            pltpu.SemaphoreType.DMA((2,)),
        ],
        name="fourier",
    )(count, offset, low_orders, mask, maps)


def plan_kernel(range_rows, device_ref, orders_ref, plan_ref):
    device = device_ref[0]
    devices = orders_ref.shape[0]
    upper = (device >= devices // 2).astype(jnp.int32)
    plan_ref[0] = orders_ref[device]
    plan_ref[1] = jnp.minimum(device, devices - 1 - device) * range_rows + upper * (range_rows // 2)
    plan_ref[2] = upper


def plan_of(device, low_orders, range_rows):
    return pl.pallas_call(
        functools.partial(plan_kernel, range_rows),
        out_shape=jax.ShapeDtypeStruct((3,), jnp.int32),
        in_specs=[SMEM_SPEC, SMEM_SPEC],
        out_specs=SMEM_SPEC,
        compiler_params=pltpu.CompilerParams(vmem_limit_bytes=VMEM_LIMIT),
        name="plan",
    )(device, low_orders)


def make_operands(given32_ref, operand_ref):
    columns = given32_ref.shape[1]
    cycles = given32_ref.shape[0] // 4
    quarter = columns // 4
    row = lax.broadcasted_iota(jnp.int32, (columns, columns), 0)
    column = lax.broadcasted_iota(jnp.int32, (columns, columns), 1)
    part = column // quarter
    hit = (row // quarter == 3 - part) & (row % quarter == column % quarter)
    sign = jnp.where((part == 1) | (part == 2), -1.0, 1.0)
    swap = jnp.where(hit, sign, 0.0).astype(jnp.bfloat16)
    for slot in range(2):
        block = given32_ref[pl.ds(slot, cycles, stride=4)].astype(jnp.bfloat16)
        lower = jnp.dot(block, swap, preferred_element_type=jnp.float32)
        operand_ref[slot, :cycles] = -block
        operand_ref[slot, cycles:] = (-lower).astype(jnp.bfloat16)


def alm_products(split, legendre_hbm, legendre_ref, operand_ref, held_ref, pad, height, sems):
    degrees = legendre_ref.shape[0]
    reads = sems.shape[0]
    for tile in range(degrees // height):
        first_row = tile * height
        place = pl.ds(first_row, height)
        if first_row % (degrees // reads) == 0:
            legendre_read(legendre_hbm, legendre_ref, sems, first_row * reads // degrees).wait()
        slot = (first_row >= split).astype(jnp.int32)
        held_ref[pad + first_row : pad + first_row + height] = jnp.dot(
            legendre_ref[place], operand_ref[slot], preferred_element_type=jnp.float32
        )
    border = pl.multiple_of(split // height * height, height)
    other = jnp.dot(legendre_ref[pl.ds(border, height)], operand_ref[1], preferred_element_type=jnp.float32)
    row_index = border + lax.broadcasted_iota(jnp.int32, (height, 1), 0)
    place = pl.ds(pad + border, height)
    held_ref[place] = jnp.where(row_index >= split, other, held_ref[place])


def legendre_read(legendre_hbm, legendre_ref, sems, part):
    size = legendre_ref.shape[0] // sems.shape[0]
    place = pl.ds(part * size, size)
    return pltpu.make_async_copy(legendre_hbm.at[place], legendre_ref.at[place], sems.at[part])


def send_kernel(
    height, plan_hbm, given_hbm, legendre_hbm, send_hbm,
    given_ref, given32_ref, operand_ref, held_ref, legendre_ref, send_ref, sems, send_sems, given_sem, plan_ref, plan_sem,
):
    plan_read = pltpu.make_async_copy(plan_hbm, plan_ref, plan_sem)
    plan_read.start()
    given_read = pltpu.make_async_copy(given_hbm, given_ref, given_sem)
    given_read.start()
    for part in range(sems.shape[0]):
        legendre_read(legendre_hbm, legendre_ref, sems, part).start()
    cycles = given_ref.shape[0] // 4
    degrees = legendre_ref.shape[0]
    plan_read.wait()
    order = plan_ref[0]
    given_read.wait()
    given32_ref[...] = given_ref[...].astype(jnp.float32)
    make_operands(given32_ref, operand_ref)
    alm_products(degrees - order, legendre_hbm, legendre_ref, operand_ref, held_ref, 32, height, sems)

    half = degrees // cycles // 2
    step = lax.broadcasted_iota(jnp.int32, (half, 1), 0)
    batch = cycles // send_sems.shape[0]
    for piece in range(send_sems.shape[0]):
        upper = piece * batch >= cycles // 2

        def one(index, carry, piece=piece, upper=upper):
            device = piece * batch + index
            block = cycles - 1 - device if upper else device
            start = pl.multiple_of(device * 2 * half, 2 * half)
            low = 2 * half * block + (half if upper else 0)
            kept = held_ref[pl.ds(32 + jnp.maximum(low - order, -half), half)]
            moved = held_ref[pl.ds(32 + degrees - jnp.minimum(low + half, order), half)]
            mirror = held_ref[pl.ds(32 + degrees - half - low - order, half)]
            mixed = jnp.where(step >= order - low, kept, moved)
            send_ref[pl.ds(start, half)] = mixed.astype(jnp.bfloat16)
            send_ref[pl.ds(start + half, half)] = mirror.astype(jnp.bfloat16)
            return carry

        lax.fori_loop(0, batch, one, 0, unroll=4)
        place = pl.ds(piece * batch * 2 * half, batch * 2 * half)
        pltpu.make_async_copy(send_ref.at[place], send_hbm.at[place], send_sems.at[piece]).start()
    for piece in range(send_sems.shape[0]):
        place = pl.ds(piece * batch * 2 * half, batch * 2 * half)
        pltpu.make_async_copy(send_ref.at[place], send_hbm.at[place], send_sems.at[piece]).wait()


def rows_to_send(plan, given, legendre, height=512):
    degrees, inner = legendre.shape
    columns = given.shape[1]
    return pl.pallas_call(
        functools.partial(send_kernel, height),
        out_shape=jax.ShapeDtypeStruct((degrees, columns), jnp.bfloat16),
        in_specs=[HBM_SPEC] * 3,
        out_specs=HBM_SPEC,
        scratch_shapes=[
            pltpu.VMEM(given.shape, jnp.bfloat16),
            pltpu.VMEM(given.shape, jnp.float32),
            pltpu.VMEM((2, inner, columns), jnp.bfloat16),
            pltpu.VMEM((degrees + 64, columns), jnp.float32),
            pltpu.VMEM((degrees, inner), jnp.bfloat16),
            pltpu.VMEM((degrees, columns), jnp.bfloat16),
            pltpu.SemaphoreType.DMA((READS,)),
            pltpu.SemaphoreType.DMA((PIECES,)),
            pltpu.SemaphoreType.DMA,
            pltpu.SMEM(plan.shape, jnp.int32),
            pltpu.SemaphoreType.DMA,
        ],
        name="rows_to_send",
    )(plan, given, legendre)


def alm_kernel(
    height, plan_ref, given_ref, legendre_hbm, alm_hbm, weight_ref, given32_ref, operand_ref, held_ref, legendre_ref, sems, sem
):
    for part in range(sems.shape[0]):
        legendre_read(legendre_hbm, legendre_ref, sems, part).start()
    given32_ref[...] = given_ref[...].astype(jnp.float32)
    make_operands(given32_ref, operand_ref)
    cycles = given_ref.shape[0] // 4
    pieces = given32_ref[pl.ds(2, cycles, stride=4)]
    lane = lax.broadcasted_iota(jnp.int32, pieces.shape, 1)
    square = jnp.sum(jnp.where(lane < 3, pieces, 0.0))
    pixels = jnp.sum(jnp.where(lane < 3, 0.0, pieces))
    weight_ref[...] = jnp.full(weight_ref.shape, square / pixels, jnp.float32)
    split = legendre_ref.shape[0] - plan_ref[0]
    alm_products(split, legendre_hbm, legendre_ref, operand_ref, held_ref, 0, height, sems)
    copy = pltpu.make_async_copy(held_ref, alm_hbm, sem)
    copy.start()
    copy.wait()


def packed_alm(plan, given, legendre, height=512):
    degrees, inner = legendre.shape
    columns = given.shape[1]
    return pl.pallas_call(
        functools.partial(alm_kernel, height),
        out_shape=(
            jax.ShapeDtypeStruct((degrees, columns), jnp.float32),
            jax.ShapeDtypeStruct((1, columns), jnp.float32),
        ),
        in_specs=[SMEM_SPEC, VMEM_SPEC, HBM_SPEC],
        out_specs=(HBM_SPEC, VMEM_SPEC),
        scratch_shapes=[
            pltpu.VMEM(given.shape, jnp.float32),
            pltpu.VMEM((2, inner, columns), jnp.bfloat16),
            pltpu.VMEM((degrees, columns), jnp.float32),
            pltpu.VMEM((degrees, inner), jnp.bfloat16),
            pltpu.SemaphoreType.DMA((READS,)),
            pltpu.SemaphoreType.DMA,
        ],
        compiler_params=pltpu.CompilerParams(vmem_limit_bytes=VMEM_LIMIT),
        name="packed_alm",
    )(plan, given, legendre)


def spectra_kernel(
    travels, degrees, plan_hbm, orders_hbm, order_row_hbm, weight_hbm, rows_hbm, out_ref,
    rows_ref, first_ref, second_ref, gram_ref, factor_ref, total_ref, sems, out_sem,
    plan_ref, order_ref, order_row_ref, weight_ref, small_sems,
):
    small = [
        pltpu.make_async_copy(source, target, small_sems.at[index])
        for index, (source, target) in enumerate(
            ((plan_hbm, plan_ref), (orders_hbm, order_ref), (order_row_hbm, order_row_ref), (weight_hbm, weight_ref))
        )
    ]
    for copy in small:
        copy.start()
    pairs = order_row_ref.shape[1]
    half = rows_ref.shape[0] // pairs // 2
    parts = sems.shape[0]
    height = rows_ref.shape[0] // parts

    def reading(part):
        place = pl.ds(part * height, height)
        return pltpu.make_async_copy(rows_hbm.at[place], rows_ref.at[place], sems.at[part])

    for part in range(parts):
        reading(part).start()
    for copy in small:
        copy.wait()
    first = plan_ref[1]
    upper = plan_ref[2] == 1
    low_wanted = upper if travels else jnp.logical_not(upper)
    step = lax.broadcasted_iota(jnp.int32, (half, 1), 0)
    columns = rows_ref.shape[1]
    quarter = columns // 4

    degree = jnp.where(low_wanted, first, degrees - half - first) + step
    orders = order_row_ref[...]
    below = (orders <= degree).astype(jnp.float32) + (degrees - orders <= degree).astype(jnp.float32)
    counts = jnp.maximum(jnp.sum(below, axis=1, keepdims=True), 1.0)
    factor_ref[...] = 2.0 / (weight_ref[...] * counts)

    def block_of(pair):
        start = pl.multiple_of(pair * 2 * half, 2 * half)
        return rows_ref[pl.ds(start, 2 * half)].astype(jnp.float32)

    def keep(pair, carry):
        early = order_ref[pair] - first
        block = jnp.where(step >= early, block_of(pair)[:half], 0.0)
        first_ref[pl.ds(pair, half, stride=PITCH)] = block
        return carry

    def move(pair, carry):
        block = block_of(pair)
        early = jnp.clip(order_ref[pair] - first, 0, half)
        first_ref[pl.ds((half - early) * PITCH + pair, half, stride=PITCH)] = block[:half]
        second_ref[pl.ds(pair, half, stride=PITCH)] = block[half:]
        return carry

    def place_rows(body):
        for part in range(parts):
            reading(part).wait()
            lax.fori_loop(part * (pairs // parts), (part + 1) * (pairs // parts), body, 0, unroll=UNROLL)

    def gram(rows):
        return lax.dot_general(rows, rows, (((0,), (0,)), ((), ())), preferred_element_type=jnp.float32)

    lane_group = lax.broadcasted_iota(jnp.int32, (8, columns), 1) // quarter

    def fold(total, index):
        for part in range(2):
            base = 2 * part * quarter
            real = total[base : base + quarter]
            imag = total[base + quarter : base + 2 * quarter]
            gram_ref[2 * index + part] = real + pltpu.roll(imag, columns - quarter, 1)

    def write_rows(step_index, carry):
        for slot in range(SLOTS):
            index = SLOTS * step_index + slot
            factor = factor_ref[pl.ds(index, 1)]
            for part in range(2):
                row = None
                for member in range(4):
                    piece = gram_ref[2 * index + part, pl.ds(member, 8, stride=4)]
                    shift = (member - 2 * part) * quarter % columns
                    if shift:
                        piece = pltpu.roll(piece, shift, 1)
                    row = piece if row is None else jnp.where(lane_group == member, piece, row)
                total_ref[pl.ds(index * 16 + part, 8, stride=2)] = row * factor
        return carry

    @pl.when(low_wanted)
    def _():
        place_rows(keep)

        def degree_step(index, carry):
            for slot in range(GRAMS):
                here = GRAMS * index + slot
                rows = first_ref[pl.ds(here * PITCH, pairs)].astype(jnp.bfloat16)
                fold(gram(rows), here)
            return carry

        lax.fori_loop(0, half // GRAMS, degree_step, 0)

    @pl.when(jnp.logical_not(low_wanted))
    def _():
        first_ref[0 : half * PITCH] = jnp.zeros((half * PITCH, columns), jnp.float32)
        place_rows(move)

        def degree_step(index, carry):
            for slot in range(GRAMS):
                here = GRAMS * index + slot
                place = pl.ds(here * PITCH, pairs)
                moved = first_ref[place].astype(jnp.bfloat16)
                mirrored = second_ref[place].astype(jnp.bfloat16)
                fold(gram(moved) + gram(mirrored), here)
            return carry

        lax.fori_loop(0, half // GRAMS, degree_step, 0)

    lax.fori_loop(0, half // SLOTS, write_rows, 0)
    if travels:
        out_ref[...] = total_ref[...].astype(out_ref.dtype)
    else:
        copy = pltpu.make_async_copy(total_ref, out_ref.at[pl.ds(0, total_ref.shape[0])], out_sem)
        copy.start()
        copy.wait()


def spectra_rows(plan, low_orders, weight, rows, travels, degrees):
    pairs = low_orders.shape[0]
    columns = rows.shape[1]
    half = rows.shape[0] // pairs // 2
    out = jax.ShapeDtypeStruct((half * (16 if travels else 32), columns), jnp.bfloat16 if travels else jnp.float32)
    return pl.pallas_call(
        functools.partial(spectra_kernel, travels, degrees),
        out_shape=out,
        in_specs=[HBM_SPEC] * 5,
        out_specs=VMEM_SPEC if travels else HBM_SPEC,
        scratch_shapes=[
            pltpu.VMEM(rows.shape, jnp.bfloat16),
            pltpu.VMEM((2 * half * PITCH, columns), jnp.float32),
            pltpu.VMEM((half * PITCH, columns), jnp.float32),
            pltpu.VMEM((2 * half, 32, columns), jnp.float32),
            pltpu.VMEM((half, columns), jnp.float32),
            pltpu.VMEM((half * 16, columns), jnp.float32),
            pltpu.SemaphoreType.DMA((PARTS,)),
            pltpu.SemaphoreType.DMA,
            pltpu.SMEM(plan.shape, jnp.int32),
            pltpu.SMEM(low_orders.shape, jnp.int32),
            pltpu.VMEM((1, pairs), jnp.int32),
            pltpu.VMEM(weight.shape, jnp.float32),
            pltpu.SemaphoreType.DMA((4,)),
        ],
        name="spectra_travel" if travels else "spectra_stay",
    )(plan, low_orders, low_orders[None], weight, rows)


def in_degree_order(rows, columns):
    tiles = rows.reshape(-1, 8, 2, columns)
    return jnp.swapaxes(tiles, 1, 2).reshape(-1, 2, 8 * columns)


def local(sky_maps, sky_mask, pixel_counts, phi_offsets, low_orders, legendre):
    devices = lax.axis_size(BAND_SUB)
    device_index = lax.axis_index(BAND_SUB)
    degree_count = legendre.shape[1]
    rows = sky_maps.shape[1] * sky_maps.shape[2]
    columns = 2 * rows
    range_rows = degree_count // devices
    outgoing = fourier(
        sky_maps.reshape(rows, sky_maps.shape[3]), sky_mask, pixel_counts, phi_offsets, low_orders[None], degree_count
    )
    received = lax.all_to_all(
        outgoing.reshape(devices, 4, columns), BAND_SUB, split_axis=0, concat_axis=0, tiled=True
    ).reshape(4 * devices, columns)
    plan = plan_of(device_index[None], low_orders, range_rows)
    send = rows_to_send(plan, received, legendre[0])
    incoming = lax.all_to_all(
        send.reshape(devices, range_rows, columns), BAND_SUB, split_axis=0, concat_axis=0, tiled=True
    ).reshape(-1, columns)
    alm, weight = packed_alm(plan, received, legendre[0])
    route = [(device, devices - 1 - device) for device in range(devices)]
    moving = spectra_rows(plan, low_orders, weight, incoming, True, degree_count)
    swapped = lax.ppermute(moving, BAND_SUB, route)
    kept = spectra_rows(plan, low_orders, weight, incoming, False, degree_count)
    spectra = lax.dynamic_update_slice_in_dim(kept, swapped.astype(jnp.float32), swapped.shape[0], 0)
    return (alm[None], in_degree_order(spectra, columns))


def solution(mesh):
    torus = Mesh(
        mesh.devices.reshape(mesh.shape["groups"], 8, 8, mesh.shape["sub"]),
        ("groups", "band_0", "band_1", "sub"),
    )
    in_specs = (
        P(GROUPS_BAND_SUB, None, None, None),
        P(GROUPS_BAND_SUB, None),
        P(GROUPS_BAND_SUB),
        P(GROUPS_BAND_SUB),
        P("groups"),
        P(GROUPS_BAND_SUB, None, None),
    )
    out_specs = (P(GROUPS_BAND_SUB, None, None), P(GROUPS_BAND_SUB, None, None))
    return jax.shard_map(local, mesh=torus, in_specs=in_specs, out_specs=out_specs, check_vma=False)
```

```python
import functools

import jax
import jax.numpy as jnp
from jax import lax
from jax.experimental import pallas as pl
from jax.experimental.pallas import tpu as pltpu
from jax.sharding import Mesh
from jax.sharding import PartitionSpec as P

BAND_SUB = ("band_0", "band_1", "sub")
GROUPS_BAND_SUB = ("groups", "band_0", "band_1", "sub")

FINE = 256
GROUP = 8
PITCH = 132
READS = 2
PIECES = 2
MAP_READS = 2
SLOTS = 16
GRAMS = 16
UNROLL = 4
VMEM_LIMIT = 67043328
ALM_VMEM = 10 * 1024 * 1024
SPECTRA_VMEM = 24 * 1024 * 1024
VMEM_SPEC = pl.BlockSpec(memory_space=pltpu.VMEM)
SMEM_SPEC = pl.BlockSpec(memory_space=pltpu.SMEM)
HBM_SPEC = pl.BlockSpec(memory_space=pltpu.HBM)


def mod_units(units, modulus, inverse):
    quotient = jnp.floor(units.astype(jnp.float32) * inverse).astype(jnp.int32)
    rest = units - quotient * modulus
    rest = jnp.where(rest < 0, rest + modulus, rest)
    return jnp.where(rest >= modulus, rest - modulus, rest)


def turn(units, modulus, inverse, scale):
    angle = scale * mod_units(units, modulus, inverse).astype(jnp.float32)
    return jnp.cos(angle), jnp.sin(angle)


def combine(first, second):
    (a_cos, a_sin), (b_cos, b_sin) = first, second
    return a_cos * b_cos - a_sin * b_sin, a_sin * b_cos + a_cos * b_sin


def fourier_kernel(
    degrees, count_ref, offset_ref, order_hbm, mask_hbm, maps_hbm, out_ref, table_ref, outer_ref, rows_ref, join_ref,
    maps_ref, sems, order_ref, mask_ref, small_sems,
):
    small = [
        pltpu.make_async_copy(source, target, small_sems.at[index])
        for index, (source, target) in enumerate(((order_hbm, order_ref), (mask_hbm, mask_ref)))
    ]
    for copy in small:
        copy.start()
    width = maps_hbm.shape[1] // sems.shape[0]
    copies = []
    for group in range(sems.shape[0]):
        place = pl.ds(group * width, width)
        copy = pltpu.make_async_copy(maps_hbm.at[:, place], maps_ref.at[:, place], sems.at[group])
        copy.start()
        copies.append(copy)
    pixel_slots = maps_ref.shape[1]
    rows = maps_ref.shape[0]
    maps_count = rows // 2
    pairs = order_ref.shape[1]
    slots = 2 * pairs
    for copy in small:
        copy.wait()
    count = count_ref[0]
    offset = offset_ref[0]
    count_float = count.astype(jnp.float32)
    modulus = 2 * count
    inverse = 1.0 / modulus.astype(jnp.float32)
    scale = jnp.pi / count_float
    low_orders = order_ref[...]
    orders = jnp.concatenate([low_orders, degrees - low_orders], axis=1)
    twice = 2 * orders
    coarse = pixel_slots // FINE
    near = 16
    step = lax.broadcasted_iota(jnp.int32, (near, slots), 0)
    low = turn(twice * step, modulus, inverse, scale)
    high = turn(twice * (near * step), modulus, inverse, scale)
    for index in range(FINE // near):
        here = tuple(part[index : index + 1] for part in high)
        cosine, sine = combine(here, low)
        table_ref[near * index : near * (index + 1), :slots] = cosine.astype(jnp.bfloat16)
        table_ref[near * index : near * (index + 1), slots:] = sine.astype(jnp.bfloat16)
    step = lax.broadcasted_iota(jnp.int32, (8, slots), 0)
    low = turn(twice * (FINE * step) + orders * offset, modulus, inverse, scale)
    high = turn(twice * (8 * FINE * step), modulus, inverse, scale)
    for index in range(coarse // 8):
        here = tuple(part[index : index + 1] for part in high)
        cosine, sine = combine(here, low)
        outer_ref[8 * index : 8 * (index + 1), :slots] = cosine
        outer_ref[8 * index : 8 * (index + 1), slots:] = sine
    pixels = lax.broadcasted_iota(jnp.int32, (1, pixel_slots), 1)
    mask = jnp.where(pixels < count, mask_ref[...], 0.0)
    square = jnp.sum(mask * mask)
    table = table_ref[...]
    real_sum = jnp.zeros((rows, slots), jnp.float32)
    imag_sum = jnp.zeros((rows, slots), jnp.float32)
    for group in range(coarse // GROUP):
        if group * GROUP * FINE % width == 0:
            copies[group * GROUP * FINE // width].wait()
        buffer = rows_ref.at[group % 2]
        for member in range(GROUP):
            first = (group * GROUP + member) * FINE
            block = maps_ref[:, first : first + FINE].astype(jnp.float32) * mask[:, first : first + FINE]
            buffer[member * rows : (member + 1) * rows, :] = block.astype(jnp.bfloat16)
        inner = jnp.dot(buffer[...], table, preferred_element_type=jnp.float32)
        for member in range(GROUP):
            index = group * GROUP + member
            cosine = outer_ref[index : index + 1, :slots]
            sine = outer_ref[index : index + 1, slots:]
            inner_cos = inner[member * rows : (member + 1) * rows, :slots]
            inner_sin = inner[member * rows : (member + 1) * rows, slots:]
            real_sum = real_sum + (cosine * inner_cos - sine * inner_sin)
            imag_sum = imag_sum + (sine * inner_cos + cosine * inner_sin)
    inverse_root = 1.0 / jnp.sqrt(count_float)
    live = twice < count
    real_part = jnp.where(live, real_sum * inverse_root, 0.0)
    imag_part = jnp.where(live, -imag_sum * inverse_root, 0.0)
    joined = jnp.concatenate(
        [real_part[:maps_count], imag_part[:maps_count], real_part[maps_count:], imag_part[maps_count:]], axis=0
    )
    join_ref[pl.ds(0, pairs, stride=4)] = jnp.transpose(joined[:, :pairs])
    join_ref[pl.ds(1, pairs, stride=4)] = jnp.transpose(joined[:, pairs:])
    lane = lax.broadcasted_iota(jnp.int32, (1, 2 * rows), 1)
    value = jnp.where(lane < 3, square, count_float)
    top = value.astype(jnp.bfloat16).astype(jnp.float32)
    middle = (value - top).astype(jnp.bfloat16).astype(jnp.float32)
    bottom = ((value - top) - middle).astype(jnp.bfloat16).astype(jnp.float32)
    kind = lane % 3
    pieces = jnp.where(kind == 0, top, jnp.where(kind == 1, middle, bottom))
    pieces = jnp.broadcast_to(jnp.where(lane < 6, pieces, 0.0), (pairs, 2 * rows))
    join_ref[pl.ds(2, pairs, stride=4)] = pieces
    join_ref[pl.ds(3, pairs, stride=4)] = pieces
    out_ref[...] = join_ref[...].astype(jnp.bfloat16)


def fourier(maps, mask, count, offset, low_orders, degrees):
    rows, pixel_slots = maps.shape
    pairs = low_orders.shape[1]
    slots = 2 * pairs
    return pl.pallas_call(
        functools.partial(fourier_kernel, degrees),
        out_shape=jax.ShapeDtypeStruct((4 * pairs, 2 * rows), jnp.bfloat16),
        in_specs=[SMEM_SPEC] * 2 + [HBM_SPEC] * 3,
        out_specs=VMEM_SPEC,
        scratch_shapes=[
            pltpu.VMEM((FINE, 2 * slots), jnp.bfloat16),
            pltpu.VMEM((pixel_slots // FINE, 2 * slots), jnp.float32),
            pltpu.VMEM((2, GROUP * rows, FINE), jnp.bfloat16),
            pltpu.VMEM((4 * pairs, 2 * rows), jnp.float32),
            pltpu.VMEM((rows, pixel_slots), jnp.bfloat16),
            pltpu.SemaphoreType.DMA((MAP_READS,)),
            pltpu.VMEM((1, pairs), jnp.int32),
            pltpu.VMEM((1, pixel_slots), jnp.float32),
            pltpu.SemaphoreType.DMA((2,)),
        ],
        name="fourier",
    )(count, offset, low_orders, mask, maps)


def plan_kernel(range_rows, device_ref, orders_ref, plan_ref):
    device = device_ref[0]
    devices = orders_ref.shape[0]
    upper = (device >= devices // 2).astype(jnp.int32)
    plan_ref[0] = orders_ref[device]
    plan_ref[1] = jnp.minimum(device, devices - 1 - device) * range_rows + upper * (range_rows // 2)
    plan_ref[2] = upper


def plan_of(device, low_orders, range_rows):
    return pl.pallas_call(
        functools.partial(plan_kernel, range_rows),
        out_shape=jax.ShapeDtypeStruct((3,), jnp.int32),
        in_specs=[SMEM_SPEC, SMEM_SPEC],
        out_specs=SMEM_SPEC,
        compiler_params=pltpu.CompilerParams(vmem_limit_bytes=VMEM_LIMIT),
        name="plan",
    )(device, low_orders)


def make_operands(given32_ref, operand_ref):
    columns = given32_ref.shape[1]
    cycles = given32_ref.shape[0] // 4
    quarter = columns // 4
    row = lax.broadcasted_iota(jnp.int32, (columns, columns), 0)
    column = lax.broadcasted_iota(jnp.int32, (columns, columns), 1)
    part = column // quarter
    hit = (row // quarter == 3 - part) & (row % quarter == column % quarter)
    sign = jnp.where((part == 1) | (part == 2), -1.0, 1.0)
    swap = jnp.where(hit, sign, 0.0).astype(jnp.bfloat16)
    for slot in range(2):
        block = given32_ref[pl.ds(slot, cycles, stride=4)].astype(jnp.bfloat16)
        lower = jnp.dot(block, swap, preferred_element_type=jnp.float32)
        operand_ref[slot, :cycles] = -block
        operand_ref[slot, cycles:] = (-lower).astype(jnp.bfloat16)


def alm_products(split, legendre_hbm, legendre_ref, operand_ref, held_ref, pad, height, sems):
    degrees = legendre_ref.shape[0]
    for tile in range(degrees // height):
        first_row = tile * height
        place = pl.ds(first_row, height)
        if sems is not None and first_row % (degrees // sems.shape[0]) == 0:
            legendre_read(legendre_hbm, legendre_ref, sems, first_row * sems.shape[0] // degrees).wait()
        slot = (first_row >= split).astype(jnp.int32)
        held_ref[pad + first_row : pad + first_row + height] = jnp.dot(
            legendre_ref[place], operand_ref[slot], preferred_element_type=jnp.float32
        )
    border = pl.multiple_of(split // height * height, height)
    other = jnp.dot(legendre_ref[pl.ds(border, height)], operand_ref[1], preferred_element_type=jnp.float32)
    row_index = border + lax.broadcasted_iota(jnp.int32, (height, 1), 0)
    place = pl.ds(pad + border, height)
    held_ref[place] = jnp.where(row_index >= split, other, held_ref[place])


def legendre_read(legendre_hbm, legendre_ref, sems, part):
    size = legendre_ref.shape[0] // sems.shape[0]
    place = pl.ds(part * size, size)
    return pltpu.make_async_copy(legendre_hbm.at[place], legendre_ref.at[place], sems.at[part])


def send_kernel(
    height, plan_hbm, given_hbm, legendre_hbm, send_hbm,
    given_ref, given32_ref, operand_ref, held_ref, legendre_ref, send_ref, sems, send_sems, given_sem, plan_ref, plan_sem,
):
    plan_read = pltpu.make_async_copy(plan_hbm, plan_ref, plan_sem)
    plan_read.start()
    given_read = pltpu.make_async_copy(given_hbm, given_ref, given_sem)
    given_read.start()
    for part in range(sems.shape[0]):
        legendre_read(legendre_hbm, legendre_ref, sems, part).start()
    cycles = given_ref.shape[0] // 4
    degrees = legendre_ref.shape[0]
    plan_read.wait()
    order = plan_ref[0]
    given_read.wait()
    given32_ref[...] = given_ref[...].astype(jnp.float32)
    make_operands(given32_ref, operand_ref)
    alm_products(degrees - order, legendre_hbm, legendre_ref, operand_ref, held_ref, 32, height, sems)

    half = degrees // cycles // 2
    step = lax.broadcasted_iota(jnp.int32, (half, 1), 0)
    batch = cycles // send_sems.shape[0]
    for piece in range(send_sems.shape[0]):
        upper = piece * batch >= cycles // 2

        def one(index, carry, piece=piece, upper=upper):
            device = piece * batch + index
            block = cycles - 1 - device if upper else device
            start = pl.multiple_of(device * 2 * half, 2 * half)
            low = 2 * half * block + (half if upper else 0)
            kept = held_ref[pl.ds(32 + jnp.maximum(low - order, -half), half)]
            moved = held_ref[pl.ds(32 + degrees - jnp.minimum(low + half, order), half)]
            mirror = held_ref[pl.ds(32 + degrees - half - low - order, half)]
            mixed = jnp.where(step >= order - low, kept, moved)
            send_ref[pl.ds(start, half)] = mixed.astype(jnp.bfloat16)
            send_ref[pl.ds(start + half, half)] = mirror.astype(jnp.bfloat16)
            return carry

        lax.fori_loop(0, batch, one, 0, unroll=4)
        place = pl.ds(piece * batch * 2 * half, batch * 2 * half)
        pltpu.make_async_copy(send_ref.at[place], send_hbm.at[place], send_sems.at[piece]).start()
    for piece in range(send_sems.shape[0]):
        place = pl.ds(piece * batch * 2 * half, batch * 2 * half)
        pltpu.make_async_copy(send_ref.at[place], send_hbm.at[place], send_sems.at[piece]).wait()


def rows_to_send(plan, given, legendre, height=512):
    degrees, inner = legendre.shape
    columns = given.shape[1]
    return pl.pallas_call(
        functools.partial(send_kernel, height),
        out_shape=jax.ShapeDtypeStruct((degrees, columns), jnp.bfloat16),
        in_specs=[HBM_SPEC] * 3,
        out_specs=HBM_SPEC,
        scratch_shapes=[
            pltpu.VMEM(given.shape, jnp.bfloat16),
            pltpu.VMEM(given.shape, jnp.float32),
            pltpu.VMEM((2, inner, columns), jnp.bfloat16),
            pltpu.VMEM((degrees + 64, columns), jnp.float32),
            pltpu.VMEM((degrees, inner), jnp.bfloat16),
            pltpu.VMEM((degrees, columns), jnp.bfloat16),
            pltpu.SemaphoreType.DMA((READS,)),
            pltpu.SemaphoreType.DMA((PIECES,)),
            pltpu.SemaphoreType.DMA,
            pltpu.SMEM(plan.shape, jnp.int32),
            pltpu.SemaphoreType.DMA,
        ],
        name="rows_to_send",
    )(plan, given, legendre)


def alm_kernel(
    height, plan_ref, given_ref, legendre_ref, alm_hbm, weight_ref, given32_ref, operand_ref, held_ref, sem
):
    given32_ref[...] = given_ref[...].astype(jnp.float32)
    make_operands(given32_ref, operand_ref)
    cycles = given_ref.shape[0] // 4
    pieces = given32_ref[pl.ds(2, cycles, stride=4)]
    lane = lax.broadcasted_iota(jnp.int32, pieces.shape, 1)
    square = jnp.sum(jnp.where(lane < 3, pieces, 0.0))
    pixels = jnp.sum(jnp.where(lane < 3, 0.0, pieces))
    weight_ref[...] = jnp.full(weight_ref.shape, square / pixels, jnp.float32)
    split = legendre_ref.shape[0] - plan_ref[0]
    alm_products(split, None, legendre_ref, operand_ref, held_ref, 0, height, None)
    copy = pltpu.make_async_copy(held_ref, alm_hbm, sem)
    copy.start()
    copy.wait()


def packed_alm(plan, given, legendre, height=512):
    degrees, inner = legendre.shape
    columns = given.shape[1]
    return pl.pallas_call(
        functools.partial(alm_kernel, height),
        out_shape=(
            jax.ShapeDtypeStruct((degrees, columns), jnp.float32),
            jax.ShapeDtypeStruct((1, columns), jnp.float32),
        ),
        in_specs=[SMEM_SPEC, VMEM_SPEC, VMEM_SPEC],
        out_specs=(HBM_SPEC, VMEM_SPEC),
        scratch_shapes=[
            pltpu.VMEM(given.shape, jnp.float32),
            pltpu.VMEM((2, inner, columns), jnp.bfloat16),
            pltpu.VMEM((degrees, columns), jnp.float32),
            pltpu.SemaphoreType.DMA,
        ],
        compiler_params=pltpu.CompilerParams(vmem_limit_bytes=ALM_VMEM),
        name="packed_alm",
    )(plan, given, legendre)


def spectra_kernel(
    travels, degrees, plan_ref, order_ref, order_row_ref, weight_ref, rows_ref, out_ref,
    first_ref, second_ref, gram_ref, factor_ref, total_ref, out_sem,
):
    pairs = order_row_ref.shape[1]
    half = rows_ref.shape[0] // pairs // 2
    first = plan_ref[1]
    upper = plan_ref[2] == 1
    low_wanted = upper if travels else jnp.logical_not(upper)
    step = lax.broadcasted_iota(jnp.int32, (half, 1), 0)
    columns = rows_ref.shape[1]
    quarter = columns // 4

    degree = jnp.where(low_wanted, first, degrees - half - first) + step
    orders = order_row_ref[...]
    below = (orders <= degree).astype(jnp.float32) + (degrees - orders <= degree).astype(jnp.float32)
    counts = jnp.maximum(jnp.sum(below, axis=1, keepdims=True), 1.0)
    factor_ref[...] = 2.0 / (weight_ref[...] * counts)

    def block_of(pair):
        start = pl.multiple_of(pair * 2 * half, 2 * half)
        return rows_ref[pl.ds(start, 2 * half)].astype(jnp.float32)

    def keep(pair, carry):
        early = order_ref[pair] - first
        block = jnp.where(step >= early, block_of(pair)[:half], 0.0)
        first_ref[pl.ds(pair, half, stride=PITCH)] = block
        return carry

    def move(pair, carry):
        block = block_of(pair)
        early = jnp.clip(order_ref[pair] - first, 0, half)
        first_ref[pl.ds((half - early) * PITCH + pair, half, stride=PITCH)] = block[:half]
        second_ref[pl.ds(pair, half, stride=PITCH)] = block[half:]
        return carry

    def place_rows(body):
        lax.fori_loop(0, pairs, body, 0, unroll=UNROLL)

    def gram(rows):
        return lax.dot_general(rows, rows, (((0,), (0,)), ((), ())), preferred_element_type=jnp.float32)

    lane_group = lax.broadcasted_iota(jnp.int32, (8, columns), 1) // quarter

    def fold(total, index):
        for part in range(2):
            base = 2 * part * quarter
            real = total[base : base + quarter]
            imag = total[base + quarter : base + 2 * quarter]
            gram_ref[2 * index + part] = real + pltpu.roll(imag, columns - quarter, 1)

    def write_rows(step_index, carry):
        for slot in range(SLOTS):
            index = SLOTS * step_index + slot
            factor = factor_ref[pl.ds(index, 1)]
            for part in range(2):
                row = None
                for member in range(4):
                    piece = gram_ref[2 * index + part, pl.ds(member, 8, stride=4)]
                    shift = (member - 2 * part) * quarter % columns
                    if shift:
                        piece = pltpu.roll(piece, shift, 1)
                    row = piece if row is None else jnp.where(lane_group == member, piece, row)
                total_ref[pl.ds(index * 16 + part, 8, stride=2)] = row * factor
        return carry

    @pl.when(low_wanted)
    def _():
        place_rows(keep)

        def degree_step(index, carry):
            for slot in range(GRAMS):
                here = GRAMS * index + slot
                rows = first_ref[pl.ds(here * PITCH, pairs)].astype(jnp.bfloat16)
                fold(gram(rows), here)
            return carry

        lax.fori_loop(0, half // GRAMS, degree_step, 0)

    @pl.when(jnp.logical_not(low_wanted))
    def _():
        first_ref[0 : half * PITCH] = jnp.zeros((half * PITCH, columns), jnp.float32)
        place_rows(move)

        def degree_step(index, carry):
            for slot in range(GRAMS):
                here = GRAMS * index + slot
                place = pl.ds(here * PITCH, pairs)
                moved = first_ref[place].astype(jnp.bfloat16)
                mirrored = second_ref[place].astype(jnp.bfloat16)
                fold(gram(moved) + gram(mirrored), here)
            return carry

        lax.fori_loop(0, half // GRAMS, degree_step, 0)

    lax.fori_loop(0, half // SLOTS, write_rows, 0)
    if travels:
        out_ref[...] = total_ref[...].astype(out_ref.dtype)
    else:
        copy = pltpu.make_async_copy(total_ref, out_ref.at[pl.ds(0, total_ref.shape[0])], out_sem)
        copy.start()
        copy.wait()


def spectra_rows(plan, low_orders, weight, rows, travels, degrees):
    pairs = low_orders.shape[0]
    columns = rows.shape[1]
    half = rows.shape[0] // pairs // 2
    out = jax.ShapeDtypeStruct((half * (16 if travels else 32), columns), jnp.bfloat16 if travels else jnp.float32)
    return pl.pallas_call(
        functools.partial(spectra_kernel, travels, degrees),
        out_shape=out,
        in_specs=[SMEM_SPEC] * 2 + [VMEM_SPEC] * 3,
        out_specs=VMEM_SPEC if travels else HBM_SPEC,
        scratch_shapes=[
            pltpu.VMEM((2 * half * PITCH, columns), jnp.float32),
            pltpu.VMEM((half * PITCH, columns), jnp.float32),
            pltpu.VMEM((2 * half, 32, columns), jnp.float32),
            pltpu.VMEM((half, columns), jnp.float32),
            pltpu.VMEM((half * 16, columns), jnp.float32),
            pltpu.SemaphoreType.DMA,
        ],
        compiler_params=pltpu.CompilerParams(vmem_limit_bytes=SPECTRA_VMEM),
        name="spectra_travel" if travels else "spectra_stay",
    )(plan, low_orders, low_orders[None], weight, rows)


def in_degree_order(rows, columns):
    tiles = rows.reshape(-1, 8, 2, columns)
    return jnp.swapaxes(tiles, 1, 2).reshape(-1, 2, 8 * columns)


def local(sky_maps, sky_mask, pixel_counts, phi_offsets, low_orders, legendre):
    devices = lax.axis_size(BAND_SUB)
    device_index = lax.axis_index(BAND_SUB)
    degree_count = legendre.shape[1]
    rows = sky_maps.shape[1] * sky_maps.shape[2]
    columns = 2 * rows
    range_rows = degree_count // devices
    outgoing = fourier(
        sky_maps.reshape(rows, sky_maps.shape[3]), sky_mask, pixel_counts, phi_offsets, low_orders[None], degree_count
    )
    received = lax.all_to_all(
        outgoing.reshape(devices, 4, columns), BAND_SUB, split_axis=0, concat_axis=0, tiled=True
    ).reshape(4 * devices, columns)
    plan = plan_of(device_index[None], low_orders, range_rows)
    send = rows_to_send(plan, received, legendre[0])
    incoming = lax.all_to_all(
        send.reshape(devices, range_rows, columns), BAND_SUB, split_axis=0, concat_axis=0, tiled=True
    ).reshape(-1, columns)
    alm, weight = packed_alm(plan, received, legendre[0])
    route = [(device, devices - 1 - device) for device in range(devices)]
    moving = spectra_rows(plan, low_orders, weight, incoming, True, degree_count)
    swapped = lax.ppermute(moving, BAND_SUB, route)
    kept = spectra_rows(plan, low_orders, weight, incoming, False, degree_count)
    spectra = lax.dynamic_update_slice_in_dim(kept, swapped.astype(jnp.float32), swapped.shape[0], 0)
    return (alm[None], in_degree_order(spectra, columns))


def solution(mesh):
    torus = Mesh(
        mesh.devices.reshape(mesh.shape["groups"], 8, 8, mesh.shape["sub"]),
        ("groups", "band_0", "band_1", "sub"),
    )
    in_specs = (
        P(GROUPS_BAND_SUB, None, None, None),
        P(GROUPS_BAND_SUB, None),
        P(GROUPS_BAND_SUB),
        P(GROUPS_BAND_SUB),
        P("groups"),
        P(GROUPS_BAND_SUB, None, None),
    )
    out_specs = (P(GROUPS_BAND_SUB, None, None), P(GROUPS_BAND_SUB, None, None))
    return jax.shard_map(local, mesh=torus, in_specs=in_specs, out_specs=out_specs, check_vma=False)
```

```python
import functools

import jax
import jax.numpy as jnp
from jax import lax
from jax.experimental import pallas as pl
from jax.experimental.pallas import tpu as pltpu
from jax.sharding import Mesh
from jax.sharding import PartitionSpec as P

BAND_SUB = ("band_0", "band_1", "sub")
GROUPS_BAND_SUB = ("groups", "band_0", "band_1", "sub")

FINE = 256
GROUP = 8
PITCH = 132
READS = 2
PIECES = 2
MAP_READS = 2
SLOTS = 16
GRAMS = 32
UNROLL = 8
PLAN_VMEM = 8 * 1024 * 1024
SEND_VMEM = 52 * 1024 * 1024
ALM_VMEM = 10 * 1024 * 1024
SPECTRA_VMEM = 24 * 1024 * 1024
VMEM_SPEC = pl.BlockSpec(memory_space=pltpu.VMEM)
SMEM_SPEC = pl.BlockSpec(memory_space=pltpu.SMEM)
HBM_SPEC = pl.BlockSpec(memory_space=pltpu.HBM)


def mod_units(units, modulus, inverse):
    quotient = jnp.floor(units.astype(jnp.float32) * inverse).astype(jnp.int32)
    rest = units - quotient * modulus
    rest = jnp.where(rest < 0, rest + modulus, rest)
    return jnp.where(rest >= modulus, rest - modulus, rest)


def turn(units, modulus, inverse, scale):
    angle = scale * mod_units(units, modulus, inverse).astype(jnp.float32)
    return jnp.cos(angle), jnp.sin(angle)


def combine(first, second):
    (a_cos, a_sin), (b_cos, b_sin) = first, second
    return a_cos * b_cos - a_sin * b_sin, a_sin * b_cos + a_cos * b_sin


def fourier_kernel(
    degrees, count_ref, offset_ref, order_hbm, mask_hbm, maps_hbm, out_ref, table_ref, outer_ref, rows_ref, join_ref,
    maps_ref, sems, order_ref, mask_ref, small_sems,
):
    small = [
        pltpu.make_async_copy(source, target, small_sems.at[index])
        for index, (source, target) in enumerate(((order_hbm, order_ref), (mask_hbm, mask_ref)))
    ]
    for copy in small:
        copy.start()
    width = maps_hbm.shape[1] // sems.shape[0]
    copies = []
    for group in range(sems.shape[0]):
        place = pl.ds(group * width, width)
        copy = pltpu.make_async_copy(maps_hbm.at[:, place], maps_ref.at[:, place], sems.at[group])
        copy.start()
        copies.append(copy)
    pixel_slots = maps_ref.shape[1]
    rows = maps_ref.shape[0]
    maps_count = rows // 2
    pairs = order_ref.shape[1]
    slots = 2 * pairs
    for copy in small:
        copy.wait()
    count = count_ref[0]
    offset = offset_ref[0]
    count_float = count.astype(jnp.float32)
    modulus = 2 * count
    inverse = 1.0 / modulus.astype(jnp.float32)
    scale = jnp.pi / count_float
    low_orders = order_ref[...]
    orders = jnp.concatenate([low_orders, degrees - low_orders], axis=1)
    twice = 2 * orders
    coarse = pixel_slots // FINE
    near = 16
    step = lax.broadcasted_iota(jnp.int32, (near, slots), 0)
    low = turn(twice * step, modulus, inverse, scale)
    high = turn(twice * (near * step), modulus, inverse, scale)
    for index in range(FINE // near):
        here = tuple(part[index : index + 1] for part in high)
        cosine, sine = combine(here, low)
        table_ref[near * index : near * (index + 1), :slots] = cosine.astype(jnp.bfloat16)
        table_ref[near * index : near * (index + 1), slots:] = sine.astype(jnp.bfloat16)
    step = lax.broadcasted_iota(jnp.int32, (8, slots), 0)
    low = turn(twice * (FINE * step) + orders * offset, modulus, inverse, scale)
    high = turn(twice * (8 * FINE * step), modulus, inverse, scale)
    for index in range(coarse // 8):
        here = tuple(part[index : index + 1] for part in high)
        cosine, sine = combine(here, low)
        outer_ref[8 * index : 8 * (index + 1), :slots] = cosine
        outer_ref[8 * index : 8 * (index + 1), slots:] = sine
    pixels = lax.broadcasted_iota(jnp.int32, (1, pixel_slots), 1)
    mask = jnp.where(pixels < count, mask_ref[...], 0.0)
    square = jnp.sum(mask * mask)
    table = table_ref[...]
    real_sum = jnp.zeros((rows, slots), jnp.float32)
    imag_sum = jnp.zeros((rows, slots), jnp.float32)
    for group in range(coarse // GROUP):
        if group * GROUP * FINE % width == 0:
            copies[group * GROUP * FINE // width].wait()
        buffer = rows_ref.at[group % 2]
        for member in range(GROUP):
            first = (group * GROUP + member) * FINE
            block = maps_ref[:, first : first + FINE].astype(jnp.float32) * mask[:, first : first + FINE]
            buffer[member * rows : (member + 1) * rows, :] = block.astype(jnp.bfloat16)
        inner = jnp.dot(buffer[...], table, preferred_element_type=jnp.float32)
        for member in range(GROUP):
            index = group * GROUP + member
            cosine = outer_ref[index : index + 1, :slots]
            sine = outer_ref[index : index + 1, slots:]
            inner_cos = inner[member * rows : (member + 1) * rows, :slots]
            inner_sin = inner[member * rows : (member + 1) * rows, slots:]
            real_sum = real_sum + (cosine * inner_cos - sine * inner_sin)
            imag_sum = imag_sum + (sine * inner_cos + cosine * inner_sin)
    inverse_root = 1.0 / jnp.sqrt(count_float)
    live = twice < count
    real_part = jnp.where(live, real_sum * inverse_root, 0.0)
    imag_part = jnp.where(live, -imag_sum * inverse_root, 0.0)
    joined = jnp.concatenate(
        [real_part[:maps_count], imag_part[:maps_count], real_part[maps_count:], imag_part[maps_count:]], axis=0
    )
    join_ref[pl.ds(0, pairs, stride=4)] = jnp.transpose(joined[:, :pairs])
    join_ref[pl.ds(1, pairs, stride=4)] = jnp.transpose(joined[:, pairs:])
    lane = lax.broadcasted_iota(jnp.int32, (1, 2 * rows), 1)
    value = jnp.where(lane < 3, square, count_float)
    top = value.astype(jnp.bfloat16).astype(jnp.float32)
    middle = (value - top).astype(jnp.bfloat16).astype(jnp.float32)
    bottom = ((value - top) - middle).astype(jnp.bfloat16).astype(jnp.float32)
    kind = lane % 3
    pieces = jnp.where(kind == 0, top, jnp.where(kind == 1, middle, bottom))
    pieces = jnp.broadcast_to(jnp.where(lane < 6, pieces, 0.0), (pairs, 2 * rows))
    join_ref[pl.ds(2, pairs, stride=4)] = pieces
    join_ref[pl.ds(3, pairs, stride=4)] = pieces
    out_ref[...] = join_ref[...].astype(jnp.bfloat16)


def fourier(maps, mask, count, offset, low_orders, degrees):
    rows, pixel_slots = maps.shape
    pairs = low_orders.shape[1]
    slots = 2 * pairs
    return pl.pallas_call(
        functools.partial(fourier_kernel, degrees),
        out_shape=jax.ShapeDtypeStruct((4 * pairs, 2 * rows), jnp.bfloat16),
        in_specs=[SMEM_SPEC] * 2 + [HBM_SPEC] * 3,
        out_specs=VMEM_SPEC,
        scratch_shapes=[
            pltpu.VMEM((FINE, 2 * slots), jnp.bfloat16),
            pltpu.VMEM((pixel_slots // FINE, 2 * slots), jnp.float32),
            pltpu.VMEM((2, GROUP * rows, FINE), jnp.bfloat16),
            pltpu.VMEM((4 * pairs, 2 * rows), jnp.float32),
            pltpu.VMEM((rows, pixel_slots), jnp.bfloat16),
            pltpu.SemaphoreType.DMA((MAP_READS,)),
            pltpu.VMEM((1, pairs), jnp.int32),
            pltpu.VMEM((1, pixel_slots), jnp.float32),
            pltpu.SemaphoreType.DMA((2,)),
        ],
        name="fourier",
    )(count, offset, low_orders, mask, maps)


def plan_kernel(range_rows, device_ref, orders_ref, plan_ref):
    device = device_ref[0]
    devices = orders_ref.shape[0]
    upper = (device >= devices // 2).astype(jnp.int32)
    plan_ref[0] = orders_ref[device]
    plan_ref[1] = jnp.minimum(device, devices - 1 - device) * range_rows + upper * (range_rows // 2)
    plan_ref[2] = upper


def plan_of(device, low_orders, range_rows):
    return pl.pallas_call(
        functools.partial(plan_kernel, range_rows),
        out_shape=jax.ShapeDtypeStruct((3,), jnp.int32),
        in_specs=[SMEM_SPEC, SMEM_SPEC],
        out_specs=SMEM_SPEC,
        compiler_params=pltpu.CompilerParams(vmem_limit_bytes=PLAN_VMEM),
        name="plan",
    )(device, low_orders)


def make_operands(given32_ref, operand_ref):
    columns = given32_ref.shape[1]
    cycles = given32_ref.shape[0] // 4
    quarter = columns // 4
    row = lax.broadcasted_iota(jnp.int32, (columns, columns), 0)
    column = lax.broadcasted_iota(jnp.int32, (columns, columns), 1)
    part = column // quarter
    hit = (row // quarter == 3 - part) & (row % quarter == column % quarter)
    sign = jnp.where((part == 1) | (part == 2), -1.0, 1.0)
    swap = jnp.where(hit, sign, 0.0).astype(jnp.bfloat16)
    for slot in range(2):
        block = given32_ref[pl.ds(slot, cycles, stride=4)].astype(jnp.bfloat16)
        lower = jnp.dot(block, swap, preferred_element_type=jnp.float32)
        operand_ref[slot, :cycles] = -block
        operand_ref[slot, cycles:] = (-lower).astype(jnp.bfloat16)


def alm_products(split, legendre_hbm, legendre_ref, operand_ref, held_ref, pad, height, sems):
    degrees = legendre_ref.shape[0]
    for tile in range(degrees // height):
        first_row = tile * height
        place = pl.ds(first_row, height)
        if sems is not None and first_row % (degrees // sems.shape[0]) == 0:
            legendre_read(legendre_hbm, legendre_ref, sems, first_row * sems.shape[0] // degrees).wait()
        slot = (first_row >= split).astype(jnp.int32)
        held_ref[pad + first_row : pad + first_row + height] = jnp.dot(
            legendre_ref[place], operand_ref[slot], preferred_element_type=jnp.float32
        )
    border = pl.multiple_of(split // height * height, height)
    other = jnp.dot(legendre_ref[pl.ds(border, height)], operand_ref[1], preferred_element_type=jnp.float32)
    row_index = border + lax.broadcasted_iota(jnp.int32, (height, 1), 0)
    place = pl.ds(pad + border, height)
    held_ref[place] = jnp.where(row_index >= split, other, held_ref[place])


def legendre_read(legendre_hbm, legendre_ref, sems, part):
    size = legendre_ref.shape[0] // sems.shape[0]
    place = pl.ds(part * size, size)
    return pltpu.make_async_copy(legendre_hbm.at[place], legendre_ref.at[place], sems.at[part])


def send_kernel(
    height, plan_ref, given_ref, legendre_hbm, send_hbm,
    given32_ref, operand_ref, held_ref, legendre_ref, send_ref, sems, send_sems,
):
    for part in range(sems.shape[0]):
        legendre_read(legendre_hbm, legendre_ref, sems, part).start()
    cycles = given_ref.shape[0] // 4
    degrees = legendre_ref.shape[0]
    order = plan_ref[0]
    given32_ref[...] = given_ref[...].astype(jnp.float32)
    make_operands(given32_ref, operand_ref)
    alm_products(degrees - order, legendre_hbm, legendre_ref, operand_ref, held_ref, 32, height, sems)

    half = degrees // cycles // 2
    step = lax.broadcasted_iota(jnp.int32, (half, 1), 0)
    batch = cycles // send_sems.shape[0]
    for piece in range(send_sems.shape[0]):
        upper = piece * batch >= cycles // 2

        def one(index, carry, piece=piece, upper=upper):
            device = piece * batch + index
            block = cycles - 1 - device if upper else device
            start = pl.multiple_of(device * 2 * half, 2 * half)
            low = 2 * half * block + (half if upper else 0)
            kept = held_ref[pl.ds(32 + jnp.maximum(low - order, -half), half)]
            moved = held_ref[pl.ds(32 + degrees - jnp.minimum(low + half, order), half)]
            mirror = held_ref[pl.ds(32 + degrees - half - low - order, half)]
            mixed = jnp.where(step >= order - low, kept, moved)
            send_ref[pl.ds(start, half)] = mixed.astype(jnp.bfloat16)
            send_ref[pl.ds(start + half, half)] = mirror.astype(jnp.bfloat16)
            return carry

        lax.fori_loop(0, batch, one, 0, unroll=4)
        place = pl.ds(piece * batch * 2 * half, batch * 2 * half)
        pltpu.make_async_copy(send_ref.at[place], send_hbm.at[place], send_sems.at[piece]).start()
    for piece in range(send_sems.shape[0]):
        place = pl.ds(piece * batch * 2 * half, batch * 2 * half)
        pltpu.make_async_copy(send_ref.at[place], send_hbm.at[place], send_sems.at[piece]).wait()


def rows_to_send(plan, given, legendre, height=512):
    degrees, inner = legendre.shape
    columns = given.shape[1]
    return pl.pallas_call(
        functools.partial(send_kernel, height),
        out_shape=jax.ShapeDtypeStruct((degrees, columns), jnp.bfloat16),
        in_specs=[SMEM_SPEC, VMEM_SPEC, HBM_SPEC],
        out_specs=HBM_SPEC,
        scratch_shapes=[
            pltpu.VMEM(given.shape, jnp.float32),
            pltpu.VMEM((2, inner, columns), jnp.bfloat16),
            pltpu.VMEM((degrees + 64, columns), jnp.float32),
            pltpu.VMEM((degrees, inner), jnp.bfloat16),
            pltpu.VMEM((degrees, columns), jnp.bfloat16),
            pltpu.SemaphoreType.DMA((READS,)),
            pltpu.SemaphoreType.DMA((PIECES,)),
        ],
        compiler_params=pltpu.CompilerParams(vmem_limit_bytes=SEND_VMEM),
        name="rows_to_send",
    )(plan, given, legendre)


def alm_kernel(
    height, plan_ref, given_ref, legendre_ref, alm_hbm, weight_ref, given32_ref, operand_ref, held_ref, sem
):
    given32_ref[...] = given_ref[...].astype(jnp.float32)
    make_operands(given32_ref, operand_ref)
    cycles = given_ref.shape[0] // 4
    pieces = given32_ref[pl.ds(2, cycles, stride=4)]
    lane = lax.broadcasted_iota(jnp.int32, pieces.shape, 1)
    square = jnp.sum(jnp.where(lane < 3, pieces, 0.0))
    pixels = jnp.sum(jnp.where(lane < 3, 0.0, pieces))
    weight_ref[...] = jnp.full(weight_ref.shape, square / pixels, jnp.float32)
    split = legendre_ref.shape[0] - plan_ref[0]
    alm_products(split, None, legendre_ref, operand_ref, held_ref, 0, height, None)
    copy = pltpu.make_async_copy(held_ref, alm_hbm, sem)
    copy.start()
    copy.wait()


def packed_alm(plan, given, legendre, height=512):
    degrees, inner = legendre.shape
    columns = given.shape[1]
    return pl.pallas_call(
        functools.partial(alm_kernel, height),
        out_shape=(
            jax.ShapeDtypeStruct((degrees, columns), jnp.float32),
            jax.ShapeDtypeStruct((1, columns), jnp.float32),
        ),
        in_specs=[SMEM_SPEC, VMEM_SPEC, VMEM_SPEC],
        out_specs=(HBM_SPEC, VMEM_SPEC),
        scratch_shapes=[
            pltpu.VMEM(given.shape, jnp.float32),
            pltpu.VMEM((2, inner, columns), jnp.bfloat16),
            pltpu.VMEM((degrees, columns), jnp.float32),
            pltpu.SemaphoreType.DMA,
        ],
        compiler_params=pltpu.CompilerParams(vmem_limit_bytes=ALM_VMEM),
        name="packed_alm",
    )(plan, given, legendre)


def spectra_kernel(
    travels, degrees, plan_ref, order_ref, order_row_ref, weight_ref, rows_ref, out_ref,
    first_ref, second_ref, gram_ref, factor_ref, total_ref, out_sem,
):
    pairs = order_row_ref.shape[1]
    half = rows_ref.shape[0] // pairs // 2
    first = plan_ref[1]
    upper = plan_ref[2] == 1
    low_wanted = upper if travels else jnp.logical_not(upper)
    step = lax.broadcasted_iota(jnp.int32, (half, 1), 0)
    columns = rows_ref.shape[1]
    quarter = columns // 4

    degree = jnp.where(low_wanted, first, degrees - half - first) + step
    orders = order_row_ref[...]
    below = (orders <= degree).astype(jnp.float32) + (degrees - orders <= degree).astype(jnp.float32)
    counts = jnp.maximum(jnp.sum(below, axis=1, keepdims=True), 1.0)
    factor_ref[...] = 2.0 / (weight_ref[...] * counts)

    def block_of(pair):
        start = pl.multiple_of(pair * 2 * half, 2 * half)
        return rows_ref[pl.ds(start, 2 * half)].astype(jnp.float32)

    def keep(pair, carry):
        early = order_ref[pair] - first
        block = jnp.where(step >= early, block_of(pair)[:half], 0.0)
        first_ref[pl.ds(pair, half, stride=PITCH)] = block
        return carry

    def move(pair, carry):
        block = block_of(pair)
        early = jnp.clip(order_ref[pair] - first, 0, half)
        first_ref[pl.ds((half - early) * PITCH + pair, half, stride=PITCH)] = block[:half]
        second_ref[pl.ds(pair, half, stride=PITCH)] = block[half:]
        return carry

    def place_rows(body):
        lax.fori_loop(0, pairs, body, 0, unroll=UNROLL)

    def gram(rows):
        return lax.dot_general(rows, rows, (((0,), (0,)), ((), ())), preferred_element_type=jnp.float32)

    lane_group = lax.broadcasted_iota(jnp.int32, (8, columns), 1) // quarter

    def fold(total, index):
        for part in range(2):
            base = 2 * part * quarter
            real = total[base : base + quarter]
            imag = total[base + quarter : base + 2 * quarter]
            gram_ref[2 * index + part] = real + pltpu.roll(imag, columns - quarter, 1)

    def write_rows(step_index, carry):
        for slot in range(SLOTS):
            index = SLOTS * step_index + slot
            factor = factor_ref[pl.ds(index, 1)]
            for part in range(2):
                row = None
                for member in range(4):
                    piece = gram_ref[2 * index + part, pl.ds(member, 8, stride=4)]
                    shift = (member - 2 * part) * quarter % columns
                    if shift:
                        piece = pltpu.roll(piece, shift, 1)
                    row = piece if row is None else jnp.where(lane_group == member, piece, row)
                total_ref[pl.ds(index * 16 + part, 8, stride=2)] = row * factor
        return carry

    @pl.when(low_wanted)
    def _():
        place_rows(keep)

        def degree_step(index, carry):
            for slot in range(GRAMS):
                here = GRAMS * index + slot
                rows = first_ref[pl.ds(here * PITCH, pairs)].astype(jnp.bfloat16)
                fold(gram(rows), here)
            return carry

        lax.fori_loop(0, half // GRAMS, degree_step, 0)

    @pl.when(jnp.logical_not(low_wanted))
    def _():
        first_ref[0 : half * PITCH] = jnp.zeros((half * PITCH, columns), jnp.float32)
        place_rows(move)

        def degree_step(index, carry):
            for slot in range(GRAMS):
                here = GRAMS * index + slot
                place = pl.ds(here * PITCH, pairs)
                moved = first_ref[place].astype(jnp.bfloat16)
                mirrored = second_ref[place].astype(jnp.bfloat16)
                fold(gram(moved) + gram(mirrored), here)
            return carry

        lax.fori_loop(0, half // GRAMS, degree_step, 0)

    lax.fori_loop(0, half // SLOTS, write_rows, 0)
    if travels:
        out_ref[...] = total_ref[...].astype(out_ref.dtype)
    else:
        copy = pltpu.make_async_copy(total_ref, out_ref.at[pl.ds(0, total_ref.shape[0])], out_sem)
        copy.start()
        copy.wait()


def spectra_rows(plan, low_orders, weight, rows, travels, degrees):
    pairs = low_orders.shape[0]
    columns = rows.shape[1]
    half = rows.shape[0] // pairs // 2
    out = jax.ShapeDtypeStruct((half * (16 if travels else 32), columns), jnp.bfloat16 if travels else jnp.float32)
    return pl.pallas_call(
        functools.partial(spectra_kernel, travels, degrees),
        out_shape=out,
        in_specs=[SMEM_SPEC] * 2 + [VMEM_SPEC] * 3,
        out_specs=VMEM_SPEC if travels else HBM_SPEC,
        scratch_shapes=[
            pltpu.VMEM((2 * half * PITCH, columns), jnp.float32),
            pltpu.VMEM((half * PITCH, columns), jnp.float32),
            pltpu.VMEM((2 * half, 32, columns), jnp.float32),
            pltpu.VMEM((half, columns), jnp.float32),
            pltpu.VMEM((half * 16, columns), jnp.float32),
            pltpu.SemaphoreType.DMA,
        ],
        compiler_params=pltpu.CompilerParams(vmem_limit_bytes=SPECTRA_VMEM),
        name="spectra_travel" if travels else "spectra_stay",
    )(plan, low_orders, low_orders[None], weight, rows)


def in_degree_order(rows, columns):
    tiles = rows.reshape(-1, 8, 2, columns)
    return jnp.swapaxes(tiles, 1, 2).reshape(-1, 2, 8 * columns)


def local(sky_maps, sky_mask, pixel_counts, phi_offsets, low_orders, legendre):
    devices = lax.axis_size(BAND_SUB)
    device_index = lax.axis_index(BAND_SUB)
    degree_count = legendre.shape[1]
    rows = sky_maps.shape[1] * sky_maps.shape[2]
    columns = 2 * rows
    range_rows = degree_count // devices
    outgoing = fourier(
        sky_maps.reshape(rows, sky_maps.shape[3]), sky_mask, pixel_counts, phi_offsets, low_orders[None], degree_count
    )
    received = lax.all_to_all(
        outgoing.reshape(devices, 4, columns), BAND_SUB, split_axis=0, concat_axis=0, tiled=True
    ).reshape(4 * devices, columns)
    plan = plan_of(device_index[None], low_orders, range_rows)
    send = rows_to_send(plan, received, legendre[0])
    incoming = lax.all_to_all(
        send.reshape(devices, range_rows, columns), BAND_SUB, split_axis=0, concat_axis=0, tiled=True
    ).reshape(-1, columns)
    alm, weight = packed_alm(plan, received, legendre[0])
    route = [(device, devices - 1 - device) for device in range(devices)]
    moving = spectra_rows(plan, low_orders, weight, incoming, True, degree_count)
    swapped = lax.ppermute(moving, BAND_SUB, route)
    kept = spectra_rows(plan, low_orders, weight, incoming, False, degree_count)
    spectra = lax.dynamic_update_slice_in_dim(kept, swapped.astype(jnp.float32), swapped.shape[0], 0)
    return (alm[None], in_degree_order(spectra, columns))


def solution(mesh):
    torus = Mesh(
        mesh.devices.reshape(mesh.shape["groups"], 8, 8, mesh.shape["sub"]),
        ("groups", "band_0", "band_1", "sub"),
    )
    in_specs = (
        P(GROUPS_BAND_SUB, None, None, None),
        P(GROUPS_BAND_SUB, None),
        P(GROUPS_BAND_SUB),
        P(GROUPS_BAND_SUB),
        P("groups"),
        P(GROUPS_BAND_SUB, None, None),
    )
    out_specs = (P(GROUPS_BAND_SUB, None, None), P(GROUPS_BAND_SUB, None, None))
    return jax.shard_map(local, mesh=torus, in_specs=in_specs, out_specs=out_specs, check_vma=False)
```

```python
import functools

import jax
import jax.numpy as jnp
from jax import lax
from jax.experimental import pallas as pl
from jax.experimental.pallas import tpu as pltpu
from jax.sharding import Mesh
from jax.sharding import PartitionSpec as P

BAND_SUB = ("band_0", "band_1", "sub")
GROUPS_BAND_SUB = ("groups", "band_0", "band_1", "sub")

FINE = 256
GROUP = 8
PITCH = 132
READS = 2
PIECES = 2
DEVICES = 4
MAP_READS = 2
SLOTS = 16
GRAMS = 32
UNROLL = 8
SEND_VMEM = 52 * 1024 * 1024
ALM_VMEM = 10 * 1024 * 1024
SPECTRA_VMEM = 24 * 1024 * 1024
VMEM_SPEC = pl.BlockSpec(memory_space=pltpu.VMEM)
SMEM_SPEC = pl.BlockSpec(memory_space=pltpu.SMEM)
HBM_SPEC = pl.BlockSpec(memory_space=pltpu.HBM)


def mod_units(units, modulus, inverse):
    quotient = jnp.floor(units.astype(jnp.float32) * inverse).astype(jnp.int32)
    rest = units - quotient * modulus
    rest = jnp.where(rest < 0, rest + modulus, rest)
    return jnp.where(rest >= modulus, rest - modulus, rest)


def turn(units, modulus, inverse, scale):
    angle = scale * mod_units(units, modulus, inverse).astype(jnp.float32)
    return jnp.cos(angle), jnp.sin(angle)


def combine(first, second):
    (a_cos, a_sin), (b_cos, b_sin) = first, second
    return a_cos * b_cos - a_sin * b_sin, a_sin * b_cos + a_cos * b_sin


def fourier_kernel(
    degrees, count_ref, offset_ref, order_hbm, mask_hbm, maps_hbm, out_ref, table_ref, outer_ref, rows_ref, join_ref,
    maps_ref, sems, order_ref, mask_ref, small_sems,
):
    small = [
        pltpu.make_async_copy(source, target, small_sems.at[index])
        for index, (source, target) in enumerate(((order_hbm, order_ref), (mask_hbm, mask_ref)))
    ]
    for copy in small:
        copy.start()
    width = maps_hbm.shape[1] // sems.shape[0]
    copies = []
    for group in range(sems.shape[0]):
        place = pl.ds(group * width, width)
        copy = pltpu.make_async_copy(maps_hbm.at[:, place], maps_ref.at[:, place], sems.at[group])
        copy.start()
        copies.append(copy)
    pixel_slots = maps_ref.shape[1]
    rows = maps_ref.shape[0]
    maps_count = rows // 2
    pairs = order_ref.shape[1]
    slots = 2 * pairs
    for copy in small:
        copy.wait()
    count = count_ref[0]
    offset = offset_ref[0]
    count_float = count.astype(jnp.float32)
    modulus = 2 * count
    inverse = 1.0 / modulus.astype(jnp.float32)
    scale = jnp.pi / count_float
    low_orders = order_ref[...]
    orders = jnp.concatenate([low_orders, degrees - low_orders], axis=1)
    twice = 2 * orders
    coarse = pixel_slots // FINE
    near = 16
    step = lax.broadcasted_iota(jnp.int32, (near, slots), 0)
    low = turn(twice * step, modulus, inverse, scale)
    high = turn(twice * (near * step), modulus, inverse, scale)
    for index in range(FINE // near):
        here = tuple(part[index : index + 1] for part in high)
        cosine, sine = combine(here, low)
        table_ref[near * index : near * (index + 1), :slots] = cosine.astype(jnp.bfloat16)
        table_ref[near * index : near * (index + 1), slots:] = sine.astype(jnp.bfloat16)
    step = lax.broadcasted_iota(jnp.int32, (8, slots), 0)
    low = turn(twice * (FINE * step) + orders * offset, modulus, inverse, scale)
    high = turn(twice * (8 * FINE * step), modulus, inverse, scale)
    for index in range(coarse // 8):
        here = tuple(part[index : index + 1] for part in high)
        cosine, sine = combine(here, low)
        outer_ref[8 * index : 8 * (index + 1), :slots] = cosine
        outer_ref[8 * index : 8 * (index + 1), slots:] = sine
    pixels = lax.broadcasted_iota(jnp.int32, (1, pixel_slots), 1)
    mask = jnp.where(pixels < count, mask_ref[...], 0.0)
    square = jnp.sum(mask * mask)
    table = table_ref[...]
    real_sum = jnp.zeros((rows, slots), jnp.float32)
    imag_sum = jnp.zeros((rows, slots), jnp.float32)
    for group in range(coarse // GROUP):
        if group * GROUP * FINE % width == 0:
            copies[group * GROUP * FINE // width].wait()
        buffer = rows_ref.at[group % 2]
        for member in range(GROUP):
            first = (group * GROUP + member) * FINE
            block = maps_ref[:, first : first + FINE].astype(jnp.float32) * mask[:, first : first + FINE]
            buffer[member * rows : (member + 1) * rows, :] = block.astype(jnp.bfloat16)
        inner = jnp.dot(buffer[...], table, preferred_element_type=jnp.float32)
        for member in range(GROUP):
            index = group * GROUP + member
            cosine = outer_ref[index : index + 1, :slots]
            sine = outer_ref[index : index + 1, slots:]
            inner_cos = inner[member * rows : (member + 1) * rows, :slots]
            inner_sin = inner[member * rows : (member + 1) * rows, slots:]
            real_sum = real_sum + (cosine * inner_cos - sine * inner_sin)
            imag_sum = imag_sum + (sine * inner_cos + cosine * inner_sin)
    inverse_root = 1.0 / jnp.sqrt(count_float)
    live = twice < count
    real_part = jnp.where(live, real_sum * inverse_root, 0.0)
    imag_part = jnp.where(live, -imag_sum * inverse_root, 0.0)
    joined = jnp.concatenate(
        [real_part[:maps_count], imag_part[:maps_count], real_part[maps_count:], imag_part[maps_count:]], axis=0
    )
    join_ref[pl.ds(0, pairs, stride=4)] = jnp.transpose(joined[:, :pairs])
    join_ref[pl.ds(1, pairs, stride=4)] = jnp.transpose(joined[:, pairs:])
    lane = lax.broadcasted_iota(jnp.int32, (1, 2 * rows), 1)
    value = jnp.where(lane < 3, square, count_float)
    top = value.astype(jnp.bfloat16).astype(jnp.float32)
    middle = (value - top).astype(jnp.bfloat16).astype(jnp.float32)
    bottom = ((value - top) - middle).astype(jnp.bfloat16).astype(jnp.float32)
    kind = lane % 3
    pieces = jnp.where(kind == 0, top, jnp.where(kind == 1, middle, bottom))
    pieces = jnp.broadcast_to(jnp.where(lane < 6, pieces, 0.0), (pairs, 2 * rows))
    join_ref[pl.ds(2, pairs, stride=4)] = pieces
    join_ref[pl.ds(3, pairs, stride=4)] = pieces
    out_ref[...] = join_ref[...].astype(jnp.bfloat16)


def fourier(maps, mask, count, offset, low_orders, degrees):
    rows, pixel_slots = maps.shape
    pairs = low_orders.shape[1]
    slots = 2 * pairs
    return pl.pallas_call(
        functools.partial(fourier_kernel, degrees),
        out_shape=jax.ShapeDtypeStruct((4 * pairs, 2 * rows), jnp.bfloat16),
        in_specs=[SMEM_SPEC] * 2 + [HBM_SPEC] * 3,
        out_specs=VMEM_SPEC,
        scratch_shapes=[
            pltpu.VMEM((FINE, 2 * slots), jnp.bfloat16),
            pltpu.VMEM((pixel_slots // FINE, 2 * slots), jnp.float32),
            pltpu.VMEM((2, GROUP * rows, FINE), jnp.bfloat16),
            pltpu.VMEM((4 * pairs, 2 * rows), jnp.float32),
            pltpu.VMEM((rows, pixel_slots), jnp.bfloat16),
            pltpu.SemaphoreType.DMA((MAP_READS,)),
            pltpu.VMEM((1, pairs), jnp.int32),
            pltpu.VMEM((1, pixel_slots), jnp.float32),
            pltpu.SemaphoreType.DMA((2,)),
        ],
        name="fourier",
    )(count, offset, low_orders, mask, maps)


def make_operands(given32_ref, operand_ref):
    columns = given32_ref.shape[1]
    cycles = given32_ref.shape[0] // 4
    quarter = columns // 4
    row = lax.broadcasted_iota(jnp.int32, (columns, columns), 0)
    column = lax.broadcasted_iota(jnp.int32, (columns, columns), 1)
    part = column // quarter
    hit = (row // quarter == 3 - part) & (row % quarter == column % quarter)
    sign = jnp.where((part == 1) | (part == 2), -1.0, 1.0)
    swap = jnp.where(hit, sign, 0.0).astype(jnp.bfloat16)
    for slot in range(2):
        block = given32_ref[pl.ds(slot, cycles, stride=4)].astype(jnp.bfloat16)
        lower = jnp.dot(block, swap, preferred_element_type=jnp.float32)
        operand_ref[slot, :cycles] = -block
        operand_ref[slot, cycles:] = (-lower).astype(jnp.bfloat16)


def alm_products(split, legendre_hbm, legendre_ref, operand_ref, held_ref, pad, height, sems):
    degrees = legendre_ref.shape[0]
    for tile in range(degrees // height):
        first_row = tile * height
        place = pl.ds(first_row, height)
        if sems is not None and first_row % (degrees // sems.shape[0]) == 0:
            legendre_read(legendre_hbm, legendre_ref, sems, first_row * sems.shape[0] // degrees).wait()
        slot = (first_row >= split).astype(jnp.int32)
        held_ref[pad + first_row : pad + first_row + height] = jnp.dot(
            legendre_ref[place], operand_ref[slot], preferred_element_type=jnp.float32
        )
    border = pl.multiple_of(split // height * height, height)
    other = jnp.dot(legendre_ref[pl.ds(border, height)], operand_ref[1], preferred_element_type=jnp.float32)
    row_index = border + lax.broadcasted_iota(jnp.int32, (height, 1), 0)
    place = pl.ds(pad + border, height)
    held_ref[place] = jnp.where(row_index >= split, other, held_ref[place])


def legendre_read(legendre_hbm, legendre_ref, sems, part):
    size = legendre_ref.shape[0] // sems.shape[0]
    place = pl.ds(part * size, size)
    return pltpu.make_async_copy(legendre_hbm.at[place], legendre_ref.at[place], sems.at[part])


def send_kernel(
    height, order_ref, given_ref, legendre_hbm, send_hbm,
    given32_ref, operand_ref, held_ref, legendre_ref, send_ref, sems, send_sems,
):
    for part in range(sems.shape[0]):
        legendre_read(legendre_hbm, legendre_ref, sems, part).start()
    cycles = given_ref.shape[0] // 4
    degrees = legendre_ref.shape[0]
    order = order_ref[0]
    given32_ref[...] = given_ref[...].astype(jnp.float32)
    make_operands(given32_ref, operand_ref)
    alm_products(degrees - order, legendre_hbm, legendre_ref, operand_ref, held_ref, 32, height, sems)

    half = degrees // cycles // 2
    step = lax.broadcasted_iota(jnp.int32, (half, 1), 0)
    batch = cycles // send_sems.shape[0]
    for piece in range(send_sems.shape[0]):
        upper = piece * batch >= cycles // 2

        def one(index, carry, piece=piece, upper=upper):
            device = piece * batch + index
            block = cycles - 1 - device if upper else device
            start = pl.multiple_of(device * 2 * half, 2 * half)
            low = 2 * half * block + (half if upper else 0)
            kept = held_ref[pl.ds(32 + jnp.maximum(low - order, -half), half)]
            moved = held_ref[pl.ds(32 + degrees - jnp.minimum(low + half, order), half)]
            mirror = held_ref[pl.ds(32 + degrees - half - low - order, half)]
            mixed = jnp.where(step >= order - low, kept, moved)
            send_ref[pl.ds(start, half)] = mixed.astype(jnp.bfloat16)
            send_ref[pl.ds(start + half, half)] = mirror.astype(jnp.bfloat16)
            return carry

        lax.fori_loop(0, batch, one, 0, unroll=DEVICES)
        place = pl.ds(piece * batch * 2 * half, batch * 2 * half)
        pltpu.make_async_copy(send_ref.at[place], send_hbm.at[place], send_sems.at[piece]).start()
    for piece in range(send_sems.shape[0]):
        place = pl.ds(piece * batch * 2 * half, batch * 2 * half)
        pltpu.make_async_copy(send_ref.at[place], send_hbm.at[place], send_sems.at[piece]).wait()


def rows_to_send(order, given, legendre, height=512):
    degrees, inner = legendre.shape
    columns = given.shape[1]
    return pl.pallas_call(
        functools.partial(send_kernel, height),
        out_shape=jax.ShapeDtypeStruct((degrees, columns), jnp.bfloat16),
        in_specs=[SMEM_SPEC, VMEM_SPEC, HBM_SPEC],
        out_specs=HBM_SPEC,
        scratch_shapes=[
            pltpu.VMEM(given.shape, jnp.float32),
            pltpu.VMEM((2, inner, columns), jnp.bfloat16),
            pltpu.VMEM((degrees + 64, columns), jnp.float32),
            pltpu.VMEM((degrees, inner), jnp.bfloat16),
            pltpu.VMEM((degrees, columns), jnp.bfloat16),
            pltpu.SemaphoreType.DMA((READS,)),
            pltpu.SemaphoreType.DMA((PIECES,)),
        ],
        compiler_params=pltpu.CompilerParams(vmem_limit_bytes=SEND_VMEM),
        name="rows_to_send",
    )(order, given, legendre)


def alm_kernel(
    height, order_ref, given_ref, legendre_ref, alm_hbm, weight_ref, given32_ref, operand_ref, held_ref, sem
):
    given32_ref[...] = given_ref[...].astype(jnp.float32)
    make_operands(given32_ref, operand_ref)
    cycles = given_ref.shape[0] // 4
    pieces = given32_ref[pl.ds(2, cycles, stride=4)]
    lane = lax.broadcasted_iota(jnp.int32, pieces.shape, 1)
    square = jnp.sum(jnp.where(lane < 3, pieces, 0.0))
    pixels = jnp.sum(jnp.where(lane < 3, 0.0, pieces))
    weight_ref[...] = jnp.full(weight_ref.shape, square / pixels, jnp.float32)
    split = legendre_ref.shape[0] - order_ref[0]
    alm_products(split, None, legendre_ref, operand_ref, held_ref, 0, height, None)
    copy = pltpu.make_async_copy(held_ref, alm_hbm, sem)
    copy.start()
    copy.wait()


def packed_alm(order, given, legendre, height=512):
    degrees, inner = legendre.shape
    columns = given.shape[1]
    return pl.pallas_call(
        functools.partial(alm_kernel, height),
        out_shape=(
            jax.ShapeDtypeStruct((degrees, columns), jnp.float32),
            jax.ShapeDtypeStruct((1, columns), jnp.float32),
        ),
        in_specs=[SMEM_SPEC, VMEM_SPEC, VMEM_SPEC],
        out_specs=(HBM_SPEC, VMEM_SPEC),
        scratch_shapes=[
            pltpu.VMEM(given.shape, jnp.float32),
            pltpu.VMEM((2, inner, columns), jnp.bfloat16),
            pltpu.VMEM((degrees, columns), jnp.float32),
            pltpu.SemaphoreType.DMA,
        ],
        compiler_params=pltpu.CompilerParams(vmem_limit_bytes=ALM_VMEM),
        name="packed_alm",
    )(order, given, legendre)


def spectra_kernel(
    travels, degrees, start_ref, upper_ref, order_ref, order_row_ref, weight_ref, rows_ref, out_ref,
    first_ref, second_ref, gram_ref, factor_ref, total_ref, out_sem,
):
    pairs = order_row_ref.shape[1]
    half = rows_ref.shape[0] // pairs // 2
    first = start_ref[0]
    upper = upper_ref[0] == 1
    low_wanted = upper if travels else jnp.logical_not(upper)
    step = lax.broadcasted_iota(jnp.int32, (half, 1), 0)
    columns = rows_ref.shape[1]
    quarter = columns // 4

    degree = jnp.where(low_wanted, first, degrees - half - first) + step
    orders = order_row_ref[...]
    below = (orders <= degree).astype(jnp.float32) + (degrees - orders <= degree).astype(jnp.float32)
    counts = jnp.maximum(jnp.sum(below, axis=1, keepdims=True), 1.0)
    factor_ref[...] = 2.0 / (weight_ref[...] * counts)

    def block_of(pair):
        start = pl.multiple_of(pair * 2 * half, 2 * half)
        return rows_ref[pl.ds(start, 2 * half)].astype(jnp.float32)

    def keep(pair, carry):
        early = order_ref[pair] - first
        block = jnp.where(step >= early, block_of(pair)[:half], 0.0)
        first_ref[pl.ds(pair, half, stride=PITCH)] = block
        return carry

    def move(pair, carry):
        block = block_of(pair)
        early = jnp.clip(order_ref[pair] - first, 0, half)
        first_ref[pl.ds((half - early) * PITCH + pair, half, stride=PITCH)] = block[:half]
        second_ref[pl.ds(pair, half, stride=PITCH)] = block[half:]
        return carry

    def place_rows(body):
        lax.fori_loop(0, pairs, body, 0, unroll=UNROLL)

    def gram(rows):
        return lax.dot_general(rows, rows, (((0,), (0,)), ((), ())), preferred_element_type=jnp.float32)

    lane_group = lax.broadcasted_iota(jnp.int32, (8, columns), 1) // quarter

    def fold(total, index):
        for part in range(2):
            base = 2 * part * quarter
            real = total[base : base + quarter]
            imag = total[base + quarter : base + 2 * quarter]
            gram_ref[2 * index + part] = real + pltpu.roll(imag, columns - quarter, 1)

    def write_rows(step_index, carry):
        for slot in range(SLOTS):
            index = SLOTS * step_index + slot
            factor = factor_ref[pl.ds(index, 1)]
            for part in range(2):
                row = None
                for member in range(4):
                    piece = gram_ref[2 * index + part, pl.ds(member, 8, stride=4)]
                    shift = (member - 2 * part) * quarter % columns
                    if shift:
                        piece = pltpu.roll(piece, shift, 1)
                    row = piece if row is None else jnp.where(lane_group == member, piece, row)
                total_ref[pl.ds(index * 16 + part, 8, stride=2)] = row * factor
        return carry

    @pl.when(low_wanted)
    def _():
        place_rows(keep)

        def degree_step(index, carry):
            for slot in range(GRAMS):
                here = GRAMS * index + slot
                rows = first_ref[pl.ds(here * PITCH, pairs)].astype(jnp.bfloat16)
                fold(gram(rows), here)
            return carry

        lax.fori_loop(0, half // GRAMS, degree_step, 0)

    @pl.when(jnp.logical_not(low_wanted))
    def _():
        first_ref[0 : half * PITCH] = jnp.zeros((half * PITCH, columns), jnp.float32)
        place_rows(move)

        def degree_step(index, carry):
            for slot in range(GRAMS):
                here = GRAMS * index + slot
                place = pl.ds(here * PITCH, pairs)
                moved = first_ref[place].astype(jnp.bfloat16)
                mirrored = second_ref[place].astype(jnp.bfloat16)
                fold(gram(moved) + gram(mirrored), here)
            return carry

        lax.fori_loop(0, half // GRAMS, degree_step, 0)

    lax.fori_loop(0, half // SLOTS, write_rows, 0)
    if travels:
        out_ref[...] = total_ref[...].astype(out_ref.dtype)
    else:
        copy = pltpu.make_async_copy(total_ref, out_ref.at[pl.ds(0, total_ref.shape[0])], out_sem)
        copy.start()
        copy.wait()


def spectra_rows(start, upper, low_orders, weight, rows, travels, degrees):
    pairs = low_orders.shape[0]
    columns = rows.shape[1]
    half = rows.shape[0] // pairs // 2
    out = jax.ShapeDtypeStruct((half * (16 if travels else 32), columns), jnp.bfloat16 if travels else jnp.float32)
    return pl.pallas_call(
        functools.partial(spectra_kernel, travels, degrees),
        out_shape=out,
        in_specs=[SMEM_SPEC] * 3 + [VMEM_SPEC] * 3,
        out_specs=VMEM_SPEC if travels else HBM_SPEC,
        scratch_shapes=[
            pltpu.VMEM((2 * half * PITCH, columns), jnp.float32),
            pltpu.VMEM((half * PITCH, columns), jnp.float32),
            pltpu.VMEM((2 * half, 32, columns), jnp.float32),
            pltpu.VMEM((half, columns), jnp.float32),
            pltpu.VMEM((half * 16, columns), jnp.float32),
            pltpu.SemaphoreType.DMA,
        ],
        compiler_params=pltpu.CompilerParams(vmem_limit_bytes=SPECTRA_VMEM),
        name="spectra_travel" if travels else "spectra_stay",
    )(start, upper, low_orders, low_orders[None], weight, rows)


def in_degree_order(rows, columns):
    tiles = rows.reshape(-1, 8, 2, columns)
    return jnp.swapaxes(tiles, 1, 2).reshape(-1, 2, 8 * columns)


def local(sky_maps, sky_mask, pixel_counts, phi_offsets, low_orders, legendre):
    devices = lax.axis_size(BAND_SUB)
    device_index = lax.axis_index(BAND_SUB)
    degree_count = legendre.shape[1]
    rows = sky_maps.shape[1] * sky_maps.shape[2]
    columns = 2 * rows
    range_rows = degree_count // devices
    outgoing = fourier(
        sky_maps.reshape(rows, sky_maps.shape[3]), sky_mask, pixel_counts, phi_offsets, low_orders[None], degree_count
    )
    received = lax.all_to_all(
        outgoing.reshape(devices, 4, columns), BAND_SUB, split_axis=0, concat_axis=0, tiled=True
    ).reshape(4 * devices, columns)
    order = lax.dynamic_slice_in_dim(low_orders, device_index, 1, 0)
    send = rows_to_send(order, received, legendre[0])
    incoming = lax.all_to_all(
        send.reshape(devices, range_rows, columns), BAND_SUB, split_axis=0, concat_axis=0, tiled=True
    ).reshape(-1, columns)
    alm, weight = packed_alm(order, received, legendre[0])
    upper = (device_index >= devices // 2).astype(jnp.int32)
    start = jnp.minimum(device_index, devices - 1 - device_index) * range_rows + upper * (range_rows // 2)
    route = [(device, devices - 1 - device) for device in range(devices)]
    moving = spectra_rows(start[None], upper[None], low_orders, weight, incoming, True, degree_count)
    swapped = lax.ppermute(moving, BAND_SUB, route)
    kept = spectra_rows(start[None], upper[None], low_orders, weight, incoming, False, degree_count)
    spectra = lax.dynamic_update_slice_in_dim(kept, swapped.astype(jnp.float32), swapped.shape[0], 0)
    return (alm[None], in_degree_order(spectra, columns))


def solution(mesh):
    torus = Mesh(
        mesh.devices.reshape(mesh.shape["groups"], 8, 8, mesh.shape["sub"]),
        ("groups", "band_0", "band_1", "sub"),
    )
    in_specs = (
        P(GROUPS_BAND_SUB, None, None, None),
        P(GROUPS_BAND_SUB, None),
        P(GROUPS_BAND_SUB),
        P(GROUPS_BAND_SUB),
        P("groups"),
        P(GROUPS_BAND_SUB, None, None),
    )
    out_specs = (P(GROUPS_BAND_SUB, None, None), P(GROUPS_BAND_SUB, None, None))
    return jax.shard_map(local, mesh=torus, in_specs=in_specs, out_specs=out_specs, check_vma=False)
```

```python
import functools

import jax
import jax.numpy as jnp
from jax import lax
from jax.experimental import pallas as pl
from jax.experimental.pallas import tpu as pltpu
from jax.sharding import Mesh
from jax.sharding import PartitionSpec as P

BAND_SUB = ("band_0", "band_1", "sub")
GROUPS_BAND_SUB = ("groups", "band_0", "band_1", "sub")

FINE = 256
GROUP = 8
PITCH = 132
READS = 2
PIECES = 2
MAP_READS = 2
SLOTS = 16
GRAMS = 32
UNROLL = 8
PLAN_VMEM = 8 * 1024 * 1024
SEND_VMEM = 52 * 1024 * 1024
ALM_VMEM = 10 * 1024 * 1024
SPECTRA_VMEM = 24 * 1024 * 1024
VMEM_SPEC = pl.BlockSpec(memory_space=pltpu.VMEM)
SMEM_SPEC = pl.BlockSpec(memory_space=pltpu.SMEM)
HBM_SPEC = pl.BlockSpec(memory_space=pltpu.HBM)


def mod_units(units, modulus, inverse):
    quotient = jnp.floor(units.astype(jnp.float32) * inverse).astype(jnp.int32)
    rest = units - quotient * modulus
    rest = jnp.where(rest < 0, rest + modulus, rest)
    return jnp.where(rest >= modulus, rest - modulus, rest)


def turn(units, modulus, inverse, scale):
    angle = scale * mod_units(units, modulus, inverse).astype(jnp.float32)
    return jnp.cos(angle), jnp.sin(angle)


def combine(first, second):
    (a_cos, a_sin), (b_cos, b_sin) = first, second
    return a_cos * b_cos - a_sin * b_sin, a_sin * b_cos + a_cos * b_sin


def fourier_kernel(
    degrees, count_ref, offset_ref, order_hbm, mask_hbm, maps_hbm, out_ref, table_ref, outer_ref, rows_ref, join_ref,
    maps_ref, sems, order_ref, mask_ref, small_sems,
):
    small = [
        pltpu.make_async_copy(source, target, small_sems.at[index])
        for index, (source, target) in enumerate(((order_hbm, order_ref), (mask_hbm, mask_ref)))
    ]
    for copy in small:
        copy.start()
    width = maps_hbm.shape[1] // sems.shape[0]
    copies = []
    for group in range(sems.shape[0]):
        place = pl.ds(group * width, width)
        copy = pltpu.make_async_copy(maps_hbm.at[:, place], maps_ref.at[:, place], sems.at[group])
        copy.start()
        copies.append(copy)
    pixel_slots = maps_ref.shape[1]
    rows = maps_ref.shape[0]
    maps_count = rows // 2
    pairs = order_ref.shape[1]
    slots = 2 * pairs
    for copy in small:
        copy.wait()
    count = count_ref[0]
    offset = offset_ref[0]
    count_float = count.astype(jnp.float32)
    modulus = 2 * count
    inverse = 1.0 / modulus.astype(jnp.float32)
    scale = jnp.pi / count_float
    low_orders = order_ref[...]
    orders = jnp.concatenate([low_orders, degrees - low_orders], axis=1)
    twice = 2 * orders
    coarse = pixel_slots // FINE
    near = 16
    step = lax.broadcasted_iota(jnp.int32, (near, slots), 0)
    low = turn(twice * step, modulus, inverse, scale)
    high = turn(twice * (near * step), modulus, inverse, scale)
    for index in range(FINE // near):
        here = tuple(part[index : index + 1] for part in high)
        cosine, sine = combine(here, low)
        table_ref[near * index : near * (index + 1), :slots] = cosine.astype(jnp.bfloat16)
        table_ref[near * index : near * (index + 1), slots:] = sine.astype(jnp.bfloat16)
    step = lax.broadcasted_iota(jnp.int32, (8, slots), 0)
    low = turn(twice * (FINE * step) + orders * offset, modulus, inverse, scale)
    high = turn(twice * (8 * FINE * step), modulus, inverse, scale)
    for index in range(coarse // 8):
        here = tuple(part[index : index + 1] for part in high)
        cosine, sine = combine(here, low)
        outer_ref[8 * index : 8 * (index + 1), :slots] = cosine
        outer_ref[8 * index : 8 * (index + 1), slots:] = sine
    pixels = lax.broadcasted_iota(jnp.int32, (1, pixel_slots), 1)
    mask = jnp.where(pixels < count, mask_ref[...], 0.0)
    square = jnp.sum(mask * mask)
    table = table_ref[...]
    real_sum = jnp.zeros((rows, slots), jnp.float32)
    imag_sum = jnp.zeros((rows, slots), jnp.float32)
    for group in range(coarse // GROUP):
        if group * GROUP * FINE % width == 0:
            copies[group * GROUP * FINE // width].wait()
        buffer = rows_ref.at[group % 2]
        for member in range(GROUP):
            first = (group * GROUP + member) * FINE
            block = maps_ref[:, first : first + FINE].astype(jnp.float32) * mask[:, first : first + FINE]
            buffer[member * rows : (member + 1) * rows, :] = block.astype(jnp.bfloat16)
        inner = jnp.dot(buffer[...], table, preferred_element_type=jnp.float32)
        for member in range(GROUP):
            index = group * GROUP + member
            cosine = outer_ref[index : index + 1, :slots]
            sine = outer_ref[index : index + 1, slots:]
            inner_cos = inner[member * rows : (member + 1) * rows, :slots]
            inner_sin = inner[member * rows : (member + 1) * rows, slots:]
            real_sum = real_sum + (cosine * inner_cos - sine * inner_sin)
            imag_sum = imag_sum + (sine * inner_cos + cosine * inner_sin)
    inverse_root = 1.0 / jnp.sqrt(count_float)
    live = twice < count
    real_part = jnp.where(live, real_sum * inverse_root, 0.0)
    imag_part = jnp.where(live, -imag_sum * inverse_root, 0.0)
    joined = jnp.concatenate(
        [real_part[:maps_count], imag_part[:maps_count], real_part[maps_count:], imag_part[maps_count:]], axis=0
    )
    join_ref[pl.ds(0, pairs, stride=4)] = jnp.transpose(joined[:, :pairs])
    join_ref[pl.ds(1, pairs, stride=4)] = jnp.transpose(joined[:, pairs:])
    lane = lax.broadcasted_iota(jnp.int32, (1, 2 * rows), 1)
    value = jnp.where(lane < 3, square, count_float)
    top = value.astype(jnp.bfloat16).astype(jnp.float32)
    middle = (value - top).astype(jnp.bfloat16).astype(jnp.float32)
    bottom = ((value - top) - middle).astype(jnp.bfloat16).astype(jnp.float32)
    kind = lane % 3
    pieces = jnp.where(kind == 0, top, jnp.where(kind == 1, middle, bottom))
    pieces = jnp.broadcast_to(jnp.where(lane < 6, pieces, 0.0), (pairs, 2 * rows))
    join_ref[pl.ds(2, pairs, stride=4)] = pieces
    join_ref[pl.ds(3, pairs, stride=4)] = pieces
    out_ref[...] = join_ref[...].astype(jnp.bfloat16)


def fourier(maps, mask, count, offset, low_orders, degrees):
    rows, pixel_slots = maps.shape
    pairs = low_orders.shape[1]
    slots = 2 * pairs
    return pl.pallas_call(
        functools.partial(fourier_kernel, degrees),
        out_shape=jax.ShapeDtypeStruct((4 * pairs, 2 * rows), jnp.bfloat16),
        in_specs=[SMEM_SPEC] * 2 + [HBM_SPEC] * 3,
        out_specs=VMEM_SPEC,
        scratch_shapes=[
            pltpu.VMEM((FINE, 2 * slots), jnp.bfloat16),
            pltpu.VMEM((pixel_slots // FINE, 2 * slots), jnp.float32),
            pltpu.VMEM((2, GROUP * rows, FINE), jnp.bfloat16),
            pltpu.VMEM((4 * pairs, 2 * rows), jnp.float32),
            pltpu.VMEM((rows, pixel_slots), jnp.bfloat16),
            pltpu.SemaphoreType.DMA((MAP_READS,)),
            pltpu.VMEM((1, pairs), jnp.int32),
            pltpu.VMEM((1, pixel_slots), jnp.float32),
            pltpu.SemaphoreType.DMA((2,)),
        ],
        name="fourier",
    )(count, offset, low_orders, mask, maps)


def plan_kernel(range_rows, device_ref, orders_ref, plan_ref):
    device = device_ref[0]
    devices = orders_ref.shape[0]
    upper = (device >= devices // 2).astype(jnp.int32)
    plan_ref[0] = orders_ref[device]
    plan_ref[1] = jnp.minimum(device, devices - 1 - device) * range_rows + upper * (range_rows // 2)
    plan_ref[2] = upper


def plan_of(device, low_orders, range_rows):
    return pl.pallas_call(
        functools.partial(plan_kernel, range_rows),
        out_shape=jax.ShapeDtypeStruct((3,), jnp.int32),
        in_specs=[SMEM_SPEC, SMEM_SPEC],
        out_specs=SMEM_SPEC,
        compiler_params=pltpu.CompilerParams(vmem_limit_bytes=PLAN_VMEM),
        name="plan",
    )(device, low_orders)


def make_operands(given32_ref, operand_ref):
    columns = given32_ref.shape[1]
    cycles = given32_ref.shape[0] // 4
    quarter = columns // 4
    row = lax.broadcasted_iota(jnp.int32, (columns, columns), 0)
    column = lax.broadcasted_iota(jnp.int32, (columns, columns), 1)
    part = column // quarter
    hit = (row // quarter == 3 - part) & (row % quarter == column % quarter)
    sign = jnp.where((part == 1) | (part == 2), -1.0, 1.0)
    swap = jnp.where(hit, sign, 0.0).astype(jnp.bfloat16)
    for slot in range(2):
        block = given32_ref[pl.ds(slot, cycles, stride=4)].astype(jnp.bfloat16)
        lower = jnp.dot(block, swap, preferred_element_type=jnp.float32)
        operand_ref[slot, :cycles] = -block
        operand_ref[slot, cycles:] = (-lower).astype(jnp.bfloat16)


def alm_products(split, legendre_hbm, legendre_ref, operand_ref, held_ref, pad, height, sems):
    degrees = legendre_ref.shape[0]
    for tile in range(degrees // height):
        first_row = tile * height
        place = pl.ds(first_row, height)
        if sems is not None and first_row % (degrees // sems.shape[0]) == 0:
            legendre_read(legendre_hbm, legendre_ref, sems, first_row * sems.shape[0] // degrees).wait()
        slot = (first_row >= split).astype(jnp.int32)
        held_ref[pad + first_row : pad + first_row + height] = jnp.dot(
            legendre_ref[place], operand_ref[slot], preferred_element_type=jnp.float32
        )
    border = pl.multiple_of(split // height * height, height)
    other = jnp.dot(legendre_ref[pl.ds(border, height)], operand_ref[1], preferred_element_type=jnp.float32)
    row_index = border + lax.broadcasted_iota(jnp.int32, (height, 1), 0)
    place = pl.ds(pad + border, height)
    held_ref[place] = jnp.where(row_index >= split, other, held_ref[place])


def legendre_read(legendre_hbm, legendre_ref, sems, part):
    size = legendre_ref.shape[0] // sems.shape[0]
    place = pl.ds(part * size, size)
    return pltpu.make_async_copy(legendre_hbm.at[place], legendre_ref.at[place], sems.at[part])


def send_kernel(
    height, orders_ref, given_ref, legendre_hbm, send_hbm,
    given32_ref, operand_ref, held_ref, legendre_ref, send_ref, sems, send_sems,
):
    for part in range(sems.shape[0]):
        legendre_read(legendre_hbm, legendre_ref, sems, part).start()
    cycles = given_ref.shape[0] // 4
    degrees = legendre_ref.shape[0]
    lane = lax.broadcasted_iota(jnp.int32, orders_ref.shape, 1)
    order = jnp.sum(jnp.where(lane == lax.axis_index(BAND_SUB), orders_ref[...], 0))
    given32_ref[...] = given_ref[...].astype(jnp.float32)
    make_operands(given32_ref, operand_ref)
    alm_products(degrees - order, legendre_hbm, legendre_ref, operand_ref, held_ref, 32, height, sems)

    half = degrees // cycles // 2
    step = lax.broadcasted_iota(jnp.int32, (half, 1), 0)
    batch = cycles // send_sems.shape[0]
    for piece in range(send_sems.shape[0]):
        upper = piece * batch >= cycles // 2

        def one(index, carry, piece=piece, upper=upper):
            device = piece * batch + index
            block = cycles - 1 - device if upper else device
            start = pl.multiple_of(device * 2 * half, 2 * half)
            low = 2 * half * block + (half if upper else 0)
            kept = held_ref[pl.ds(32 + jnp.maximum(low - order, -half), half)]
            moved = held_ref[pl.ds(32 + degrees - jnp.minimum(low + half, order), half)]
            mirror = held_ref[pl.ds(32 + degrees - half - low - order, half)]
            mixed = jnp.where(step >= order - low, kept, moved)
            send_ref[pl.ds(start, half)] = mixed.astype(jnp.bfloat16)
            send_ref[pl.ds(start + half, half)] = mirror.astype(jnp.bfloat16)
            return carry

        lax.fori_loop(0, batch, one, 0, unroll=4)
        place = pl.ds(piece * batch * 2 * half, batch * 2 * half)
        pltpu.make_async_copy(send_ref.at[place], send_hbm.at[place], send_sems.at[piece]).start()
    for piece in range(send_sems.shape[0]):
        place = pl.ds(piece * batch * 2 * half, batch * 2 * half)
        pltpu.make_async_copy(send_ref.at[place], send_hbm.at[place], send_sems.at[piece]).wait()


def rows_to_send(low_orders, given, legendre, height=512):
    degrees, inner = legendre.shape
    columns = given.shape[1]
    return pl.pallas_call(
        functools.partial(send_kernel, height),
        out_shape=jax.ShapeDtypeStruct((degrees, columns), jnp.bfloat16),
        in_specs=[VMEM_SPEC, VMEM_SPEC, HBM_SPEC],
        out_specs=HBM_SPEC,
        scratch_shapes=[
            pltpu.VMEM(given.shape, jnp.float32),
            pltpu.VMEM((2, inner, columns), jnp.bfloat16),
            pltpu.VMEM((degrees + 64, columns), jnp.float32),
            pltpu.VMEM((degrees, inner), jnp.bfloat16),
            pltpu.VMEM((degrees, columns), jnp.bfloat16),
            pltpu.SemaphoreType.DMA((READS,)),
            pltpu.SemaphoreType.DMA((PIECES,)),
        ],
        compiler_params=pltpu.CompilerParams(vmem_limit_bytes=SEND_VMEM),
        name="rows_to_send",
    )(low_orders, given, legendre)


def alm_kernel(
    height, plan_ref, given_ref, legendre_ref, alm_hbm, weight_ref, given32_ref, operand_ref, held_ref, sem
):
    given32_ref[...] = given_ref[...].astype(jnp.float32)
    make_operands(given32_ref, operand_ref)
    cycles = given_ref.shape[0] // 4
    pieces = given32_ref[pl.ds(2, cycles, stride=4)]
    lane = lax.broadcasted_iota(jnp.int32, pieces.shape, 1)
    square = jnp.sum(jnp.where(lane < 3, pieces, 0.0))
    pixels = jnp.sum(jnp.where(lane < 3, 0.0, pieces))
    weight_ref[...] = jnp.full(weight_ref.shape, square / pixels, jnp.float32)
    split = legendre_ref.shape[0] - plan_ref[0]
    alm_products(split, None, legendre_ref, operand_ref, held_ref, 0, height, None)
    copy = pltpu.make_async_copy(held_ref, alm_hbm, sem)
    copy.start()
    copy.wait()


def packed_alm(plan, given, legendre, height=512):
    degrees, inner = legendre.shape
    columns = given.shape[1]
    return pl.pallas_call(
        functools.partial(alm_kernel, height),
        out_shape=(
            jax.ShapeDtypeStruct((degrees, columns), jnp.float32),
            jax.ShapeDtypeStruct((1, columns), jnp.float32),
        ),
        in_specs=[SMEM_SPEC, VMEM_SPEC, VMEM_SPEC],
        out_specs=(HBM_SPEC, VMEM_SPEC),
        scratch_shapes=[
            pltpu.VMEM(given.shape, jnp.float32),
            pltpu.VMEM((2, inner, columns), jnp.bfloat16),
            pltpu.VMEM((degrees, columns), jnp.float32),
            pltpu.SemaphoreType.DMA,
        ],
        compiler_params=pltpu.CompilerParams(vmem_limit_bytes=ALM_VMEM),
        name="packed_alm",
    )(plan, given, legendre)


def spectra_kernel(
    travels, degrees, plan_ref, order_ref, order_row_ref, weight_ref, rows_ref, out_ref,
    first_ref, second_ref, gram_ref, factor_ref, total_ref, out_sem,
):
    pairs = order_row_ref.shape[1]
    half = rows_ref.shape[0] // pairs // 2
    first = plan_ref[1]
    upper = plan_ref[2] == 1
    low_wanted = upper if travels else jnp.logical_not(upper)
    step = lax.broadcasted_iota(jnp.int32, (half, 1), 0)
    columns = rows_ref.shape[1]
    quarter = columns // 4

    degree = jnp.where(low_wanted, first, degrees - half - first) + step
    orders = order_row_ref[...]
    below = (orders <= degree).astype(jnp.float32) + (degrees - orders <= degree).astype(jnp.float32)
    counts = jnp.maximum(jnp.sum(below, axis=1, keepdims=True), 1.0)
    factor_ref[...] = 2.0 / (weight_ref[...] * counts)

    def block_of(pair):
        start = pl.multiple_of(pair * 2 * half, 2 * half)
        return rows_ref[pl.ds(start, 2 * half)].astype(jnp.float32)

    def keep(pair, carry):
        early = order_ref[pair] - first
        block = jnp.where(step >= early, block_of(pair)[:half], 0.0)
        first_ref[pl.ds(pair, half, stride=PITCH)] = block
        return carry

    def move(pair, carry):
        block = block_of(pair)
        early = jnp.clip(order_ref[pair] - first, 0, half)
        first_ref[pl.ds((half - early) * PITCH + pair, half, stride=PITCH)] = block[:half]
        second_ref[pl.ds(pair, half, stride=PITCH)] = block[half:]
        return carry

    def place_rows(body):
        lax.fori_loop(0, pairs, body, 0, unroll=UNROLL)

    def gram(rows):
        return lax.dot_general(rows, rows, (((0,), (0,)), ((), ())), preferred_element_type=jnp.float32)

    lane_group = lax.broadcasted_iota(jnp.int32, (8, columns), 1) // quarter

    def fold(total, index):
        for part in range(2):
            base = 2 * part * quarter
            real = total[base : base + quarter]
            imag = total[base + quarter : base + 2 * quarter]
            gram_ref[2 * index + part] = real + pltpu.roll(imag, columns - quarter, 1)

    def write_rows(step_index, carry):
        for slot in range(SLOTS):
            index = SLOTS * step_index + slot
            factor = factor_ref[pl.ds(index, 1)]
            for part in range(2):
                row = None
                for member in range(4):
                    piece = gram_ref[2 * index + part, pl.ds(member, 8, stride=4)]
                    shift = (member - 2 * part) * quarter % columns
                    if shift:
                        piece = pltpu.roll(piece, shift, 1)
                    row = piece if row is None else jnp.where(lane_group == member, piece, row)
                total_ref[pl.ds(index * 16 + part, 8, stride=2)] = row * factor
        return carry

    @pl.when(low_wanted)
    def _():
        place_rows(keep)

        def degree_step(index, carry):
            for slot in range(GRAMS):
                here = GRAMS * index + slot
                rows = first_ref[pl.ds(here * PITCH, pairs)].astype(jnp.bfloat16)
                fold(gram(rows), here)
            return carry

        lax.fori_loop(0, half // GRAMS, degree_step, 0)

    @pl.when(jnp.logical_not(low_wanted))
    def _():
        first_ref[0 : half * PITCH] = jnp.zeros((half * PITCH, columns), jnp.float32)
        place_rows(move)

        def degree_step(index, carry):
            for slot in range(GRAMS):
                here = GRAMS * index + slot
                place = pl.ds(here * PITCH, pairs)
                moved = first_ref[place].astype(jnp.bfloat16)
                mirrored = second_ref[place].astype(jnp.bfloat16)
                fold(gram(moved) + gram(mirrored), here)
            return carry

        lax.fori_loop(0, half // GRAMS, degree_step, 0)

    lax.fori_loop(0, half // SLOTS, write_rows, 0)
    if travels:
        out_ref[...] = total_ref[...].astype(out_ref.dtype)
    else:
        copy = pltpu.make_async_copy(total_ref, out_ref.at[pl.ds(0, total_ref.shape[0])], out_sem)
        copy.start()
        copy.wait()


def spectra_rows(plan, low_orders, weight, rows, travels, degrees):
    pairs = low_orders.shape[0]
    columns = rows.shape[1]
    half = rows.shape[0] // pairs // 2
    out = jax.ShapeDtypeStruct((half * (16 if travels else 32), columns), jnp.bfloat16 if travels else jnp.float32)
    return pl.pallas_call(
        functools.partial(spectra_kernel, travels, degrees),
        out_shape=out,
        in_specs=[SMEM_SPEC] * 2 + [VMEM_SPEC] * 3,
        out_specs=VMEM_SPEC if travels else HBM_SPEC,
        scratch_shapes=[
            pltpu.VMEM((2 * half * PITCH, columns), jnp.float32),
            pltpu.VMEM((half * PITCH, columns), jnp.float32),
            pltpu.VMEM((2 * half, 32, columns), jnp.float32),
            pltpu.VMEM((half, columns), jnp.float32),
            pltpu.VMEM((half * 16, columns), jnp.float32),
            pltpu.SemaphoreType.DMA,
        ],
        compiler_params=pltpu.CompilerParams(vmem_limit_bytes=SPECTRA_VMEM),
        name="spectra_travel" if travels else "spectra_stay",
    )(plan, low_orders, low_orders[None], weight, rows)


def in_degree_order(rows, columns):
    tiles = rows.reshape(-1, 8, 2, columns)
    return jnp.swapaxes(tiles, 1, 2).reshape(-1, 2, 8 * columns)


def local(sky_maps, sky_mask, pixel_counts, phi_offsets, low_orders, legendre):
    devices = lax.axis_size(BAND_SUB)
    device_index = lax.axis_index(BAND_SUB)
    degree_count = legendre.shape[1]
    rows = sky_maps.shape[1] * sky_maps.shape[2]
    columns = 2 * rows
    range_rows = degree_count // devices
    outgoing = fourier(
        sky_maps.reshape(rows, sky_maps.shape[3]), sky_mask, pixel_counts, phi_offsets, low_orders[None], degree_count
    )
    received = lax.all_to_all(
        outgoing.reshape(devices, 4, columns), BAND_SUB, split_axis=0, concat_axis=0, tiled=True
    ).reshape(4 * devices, columns)
    plan = plan_of(device_index[None], low_orders, range_rows)
    send = rows_to_send(low_orders[None], received, legendre[0])
    incoming = lax.all_to_all(
        send.reshape(devices, range_rows, columns), BAND_SUB, split_axis=0, concat_axis=0, tiled=True
    ).reshape(-1, columns)
    alm, weight = packed_alm(plan, received, legendre[0])
    route = [(device, devices - 1 - device) for device in range(devices)]
    moving = spectra_rows(plan, low_orders, weight, incoming, True, degree_count)
    swapped = lax.ppermute(moving, BAND_SUB, route)
    kept = spectra_rows(plan, low_orders, weight, incoming, False, degree_count)
    spectra = lax.dynamic_update_slice_in_dim(kept, swapped.astype(jnp.float32), swapped.shape[0], 0)
    return (alm[None], in_degree_order(spectra, columns))


def solution(mesh):
    torus = Mesh(
        mesh.devices.reshape(mesh.shape["groups"], 8, 8, mesh.shape["sub"]),
        ("groups", "band_0", "band_1", "sub"),
    )
    in_specs = (
        P(GROUPS_BAND_SUB, None, None, None),
        P(GROUPS_BAND_SUB, None),
        P(GROUPS_BAND_SUB),
        P(GROUPS_BAND_SUB),
        P("groups"),
        P(GROUPS_BAND_SUB, None, None),
    )
    out_specs = (P(GROUPS_BAND_SUB, None, None), P(GROUPS_BAND_SUB, None, None))
    return jax.shard_map(local, mesh=torus, in_specs=in_specs, out_specs=out_specs, check_vma=False)
```
